32 devices in a mesh: zon: 8 (over z, y), mer: 4 (over x, core).
Axes of the slice: x: 2, y: 2, z: 4, core: 2. Of those that a mesh axis runs over, the one named last changes fastest.
Arguments:
- sea_level: float32 [512, 4096], P('mer', 'zon'), may hold values from -6 to 6
- forcing: float32 [512, 4096], P('mer', 'zon'), may hold values from -6 to 6
- link_weights: float32 [8, 512, 4096], P(None, 'mer', 'zon'), may hold values from 0.1 to 2
- excess: float32 [512, 4096], P('mer', 'zon'), may hold values from 0.05 to 0.5
- ocean_mask: int32 [512, 4096], P('mer', 'zon'), may hold values 0 or 1
- current: float32 [2, 512, 4096], P(None, 'mer', 'zon'), may hold values from -6 to 6
- intersection_block: int32 [32, 32, 32], P(('zon', 'mer')), may hold values from -1 to 511, as said below
- intersection_cols: int32 [32, 32, 32, 128], P(('zon', 'mer')), may hold values from -1 to 127, as said below
- ice_mass: float32 [32, 32, 32, 128], P(('zon', 'mer')), may hold values from 0.2 to 3
- coriolis: float32 [32, 32, 32, 128], P(('zon', 'mer')), may hold values from -1.5 to 1.5
- ice_start: float32 [2, 32, 32, 32, 128], P(None, ('zon', 'mer')), may hold values from -6 to 6
- wind_stress: float32 [2, 32, 32, 32, 128], P(None, ('zon', 'mer')), may hold values from -6 to 6
Outputs:
- surface: float32 [512, 4096], P('mer', 'zon')
- velocity: float32 [2, 32, 32, 32, 128], P(None, ('zon', 'mer'))
The draws below stay inside these ranges and needn't reach their ends.
Inputs may be any that keep to these rules, and one draw needn't show every extreme that they name: `intersection_block`: for each owner device and ice device, the live ocean block numbers come first among the 32 slots and empty slots hold -1; in every draw one ice device receives 32 live blocks from every owner device. `intersection_cols`: within a live intersection block the cells named by different rows are distinct; rows of empty slots are all -1.
All inputs are finite; a program needn't handle non-finite values. No bound on the sum of `ocean_mask` on one device may be relied on, other than what follows from the above.
Results may differ from the reference program's by a relative error of at most 0.00002.
Values sent between devices are 32-bit elements; how exact they have to be, the bound alone decides.
A program may use at most 256 MiB of HBM per device.

```python
import math
import jax
import jax.numpy as jnp
from jax import lax

LAT_DEV = 128
LON_DEV = 512
BLOCK = 128
SWEEPS = 2
ICE_SWEEPS = 3
NY = 512
NX = 4096
OCEAN_BLOCKS = 512
PAIR_SLOTS = 32
N_ZON = 8
N_MER = 4
DEVICES = 32


def intersection_lists(key):
    base = jax.random.fold_in(key, 7)
    subkeys = jax.random.split(base, 5)
    counts = jax.random.randint(subkeys[0], (DEVICES, DEVICES), 0, PAIR_SLOTS + 1)
    full_target = jax.random.randint(subkeys[1], (), 0, DEVICES)
    ice_index = jnp.arange(DEVICES)
    counts = jnp.where(ice_index[None, :] == full_target, PAIR_SLOTS, counts)
    empty_target = (full_target + 1) % DEVICES
    counts = counts.at[0, empty_target].set(0)
    slot_index = jnp.arange(PAIR_SLOTS)
    is_live = slot_index[None, None, :] < counts[:, :, None]
    chosen = jax.random.randint(subkeys[2], (DEVICES, DEVICES, PAIR_SLOTS), 0, OCEAN_BLOCKS)
    chosen = chosen.at[0, full_target, 0].set(OCEAN_BLOCKS - 1)
    blocks = jnp.where(is_live, chosen, -1)
    scores = jax.random.randint(subkeys[3], (DEVICES, DEVICES, PAIR_SLOTS, BLOCK), 0, 1 << 20) * BLOCK + jnp.arange(BLOCK)
    shuffled = jnp.argsort(scores, axis=-1).astype(jnp.int32)
    keep_row = jax.random.randint(subkeys[4], (DEVICES, DEVICES, PAIR_SLOTS, BLOCK), 0, 8) > 0
    columns = jnp.where(is_live[..., None] & keep_row, shuffled, -1)
    return (blocks.astype(jnp.int32), columns.astype(jnp.int32))


def draw_intersection_block(key, part):
    return intersection_lists(key)[0]


def draw_intersection_cols(key, part):
    return intersection_lists(key)[1]


def set_ends(entries, stream_key, low, top_value):
    longest = entries.shape.index(max(entries.shape))
    spots = []
    for shift in (0, 1):
        where = [jax.random.randint(jax.random.fold_in(stream_key, axis), (), 0, length) for axis, length in enumerate(entries.shape)]
        where[longest] = (where[longest] + shift) % entries.shape[longest]
        spots.append(tuple(where))
    return entries.at[spots[0]].set(low).at[spots[1]].set(top_value)


def block_scale(own_key, shape, cuts, smallest, high):
    gain = 1.0
    for axis_at, parts in cuts:
        steps = jax.random.uniform(jax.random.fold_in(jax.random.fold_in(own_key, 6), axis_at), (parts,), jnp.float32, smallest / len(cuts), high / len(cuts))
        gain = gain * jnp.repeat(jnp.exp(steps), shape[axis_at] // parts).reshape((-1,) + (1,) * (len(shape) - 1 - axis_at))
    return gain


def noise(stream_key, shape, deviation, limit, cuts=(), kind=jnp.bfloat16):
    array = deviation * jax.random.normal(stream_key, shape, jnp.float32)
    if cuts:
        array = array * block_scale(stream_key, shape, cuts, -0.22, 0.18)
    return jnp.clip(array, -limit, limit).astype(kind)


def setup_inputs(seed: int = 0) -> dict:
    splits = jax.random.split(jax.random.key(seed), 13)
    return {
        "sea_level": noise(splits[0], (NY, NX), 1.0, 6.0, ((0, 4), (1, 8)), jnp.float32),
        "forcing": noise(splits[1], (NY, NX), 1.0, 6.0, ((0, 4), (1, 8)), jnp.float32),
        "link_weights": jnp.clip(jnp.exp(math.log(2.0) - 2.9957323 * jax.random.uniform(splits[2], (8, NY, NX), jnp.float32) ** block_scale(splits[2], (8, NY, NX), ((1, 4), (2, 8)), -0.2, 0.2)), 0.1, 2.0),
        "excess": jnp.clip(jnp.exp(math.log(0.5) - 2.3025851 * jax.random.uniform(splits[3], (NY, NX), jnp.float32) ** block_scale(splits[3], (NY, NX), ((0, 4), (1, 8)), -0.2, 0.2)), 0.05, 0.5),
        "ocean_mask": set_ends((jax.random.randint(splits[4], (NY, NX), 0, 8) < 7).astype(jnp.int32), jax.random.fold_in(splits[4], 1), 0, 1),
        "current": noise(splits[5], (2, NY, NX), 1.0, 6.0, ((1, 4), (2, 8)), jnp.float32),
        "intersection_block": draw_intersection_block(jax.random.fold_in(splits[12], 71), 0),
        "intersection_cols": draw_intersection_cols(jax.random.fold_in(splits[12], 71), 0),
        "ice_mass": jnp.clip(jnp.exp(math.log(3.0) - 2.7080502 * jax.random.uniform(splits[8], (DEVICES, DEVICES, PAIR_SLOTS, BLOCK), jnp.float32) ** block_scale(splits[8], (DEVICES, DEVICES, PAIR_SLOTS, BLOCK), ((0, 32),), -0.2, 0.2)), 0.2, 3.0),
        "coriolis": jnp.clip(jax.random.uniform(splits[9], (DEVICES, DEVICES, PAIR_SLOTS, BLOCK), jnp.float32, -1.5, 1.5) * block_scale(splits[9], (DEVICES, DEVICES, PAIR_SLOTS, BLOCK), ((0, 32),), -0.4, 0.0), -1.5, 1.5),
        "ice_start": noise(splits[10], (2, DEVICES, DEVICES, PAIR_SLOTS, BLOCK), 1.0, 6.0, ((1, 32),), jnp.float32),
        "wind_stress": noise(splits[11], (2, DEVICES, DEVICES, PAIR_SLOTS, BLOCK), 1.0, 6.0, ((1, 32),), jnp.float32),
    }


drag_coeff = 1.0
link_coeff = 0.5
neighbour_steps = ((0, 1), (0, -1), (1, 0), (-1, 0), (1, 1), (1, -1), (-1, 1), (-1, -1))


def colour_sequence(sweep_count):
    return [0] + [1, 2, 3, 2, 1, 0] * sweep_count


def gauss_seidel(surface, source, link_weights, diagonal, is_ocean, pad_fn):
    row_count, col_count = surface.shape
    row_parity = lax.broadcasted_iota(jnp.int32, (row_count, col_count), 0) % 2
    col_parity = lax.broadcasted_iota(jnp.int32, (row_count, col_count), 1) % 2
    colours = 2 * row_parity + col_parity
    for colour in colour_sequence(SWEEPS):
        padded = pad_fn(surface)
        gathered = source
        for position, (row_step, col_step) in enumerate(neighbour_steps):
            gathered = gathered + link_weights[position] * padded[1 + row_step:1 + row_step + row_count, 1 + col_step:1 + col_step + col_count]
        surface = jnp.where(is_ocean & (colours == colour), gathered / diagonal, surface)
    return surface


def pad_whole(surface):
    wrapped = jnp.concatenate([surface[:, -1:], surface, surface[:, :1]], axis=1)
    return jnp.pad(wrapped, ((1, 1), (0, 0)))


def along_block(values):
    padded = jnp.pad(values, [(0, 0)] * (values.ndim - 1) + [(1, 1)])
    return padded[..., :-2] + padded[..., 2:]


def ice_momentum(ice_mass, coriolis, ice_start, wind_stress, current):
    diagonal = ice_mass + drag_coeff + 2.0 * link_coeff
    turning = coriolis * ice_mass
    determinant = diagonal * diagonal + turning * turning
    base_east = ice_mass * ice_start[0] + wind_stress[0] + drag_coeff * current[0]
    base_north = ice_mass * ice_start[1] + wind_stress[1] + drag_coeff * current[1]
    velocity = ice_start
    for sweep_index in range(ICE_SWEEPS):
        beside = along_block(velocity)
        right_east = base_east + link_coeff * beside[0]
        right_north = base_north + link_coeff * beside[1]
        velocity = jnp.stack([(diagonal * right_east + turning * right_north) / determinant,
                              (diagonal * right_north - turning * right_east) / determinant])
    return velocity


def reference(sea_level, forcing, link_weights, excess, ocean_mask, current, intersection_block, intersection_cols, ice_mass, coriolis, ice_start, wind_stress):
    blocks = current.reshape(2, N_MER, LAT_DEV, N_ZON, LON_DEV).transpose(0, 3, 1, 2, 4).reshape(2, DEVICES, OCEAN_BLOCKS, BLOCK)
    owners = jnp.arange(DEVICES, dtype=jnp.int32)[:, None, None]
    picked = blocks[:, owners, jnp.maximum(intersection_block, 0).astype(jnp.int32)]
    valid = intersection_cols >= 0
    values = jnp.take_along_axis(picked, jnp.maximum(intersection_cols, 0)[None], axis=4)
    values = jnp.where(valid[None], values, 0.0)
    ice_current = values.transpose(0, 2, 1, 3, 4)
    velocity = ice_momentum(ice_mass, coriolis, ice_start, wind_stress, ice_current)
    ice_drag = drag_coeff * (velocity - ice_current)
    owner_drag = ice_drag.transpose(2, 0, 1, 3, 4)
    target = jnp.where(valid, jnp.maximum(intersection_block, 0)[..., None] * BLOCK + intersection_cols, OCEAN_BLOCKS * BLOCK).astype(jnp.int32)

    def scatter_owner(pair):
        owner_target, owner_values = pair
        return jnp.zeros((2, OCEAN_BLOCKS * BLOCK), jnp.float32).at[:, owner_target.reshape(-1)].add(owner_values.reshape(2, -1), mode="drop")

    summed = lax.map(scatter_owner, (target, owner_drag))
    stress_grid = summed.reshape(N_ZON, N_MER, 2, LAT_DEV, LON_DEV).transpose(2, 1, 3, 0, 4).reshape(2, N_MER * LAT_DEV, N_ZON * LON_DEV)
    stress_north = stress_grid[1]
    zonal_diff = jnp.roll(stress_north, -1, axis=1) - jnp.roll(stress_north, 1, axis=1)
    padded_east = jnp.pad(stress_grid[0], ((1, 1), (0, 0)))
    meridional_diff = padded_east[2:] - padded_east[:-2]
    source = forcing + zonal_diff - meridional_diff
    is_ocean = ocean_mask > 0
    diagonal = jnp.where(is_ocean, (1.0 + excess) * jnp.sum(link_weights, axis=0), 1.0)
    surface = jnp.where(is_ocean, sea_level, 0.0)
    surface = gauss_seidel(surface, source, link_weights, diagonal, is_ocean, pad_whole)
    return surface, velocity
```

```python
import functools

import jax
import jax.numpy as jnp
from jax import lax
from jax.experimental import pallas as pl
from jax.experimental.pallas import tpu as pltpu
from jax.sharding import PartitionSpec as P

SWEEPS = 2
ICE_SWEEPS = 3
ROW_RIM = 8
COL_RIM = 16
LANES = 128

drag_coeff = 1.0
link_coeff = 0.5
VM = pl.BlockSpec(memory_space=pltpu.VMEM)
HBM = pl.BlockSpec(memory_space=pltpu.HBM)
TRAVEL_VMEM = 40 * 1024 * 1024
SWEEP_VMEM = 16 * 1024 * 1024


def cost(flops, nbytes):
    return pl.CostEstimate(flops=flops, bytes_accessed=nbytes, transcendentals=0)


def lane_take(values, index):
    return jnp.take_along_axis(values, index, axis=1, mode="promise_in_bounds")


def split3(values):
    high = values.astype(jnp.bfloat16)
    rest = values - high.astype(jnp.float32)
    middle = rest.astype(jnp.bfloat16)
    low = (rest - middle.astype(jnp.float32)).astype(jnp.bfloat16)
    return high, middle, low


def nn_dot(a, b):
    return lax.dot_general(a, b, (((1,), (0,)), ((), ())), preferred_element_type=jnp.float32)


def block_rows(blocks, tiles, rows):
    safe = jnp.maximum(blocks, 0)
    return jnp.where(blocks >= 0, (safe % tiles) * rows + safe // tiles, -1)


def inverse_rows(cols):
    lane = lax.broadcasted_iota(jnp.int32, (8, LANES), 1)
    sub = lax.broadcasted_iota(jnp.int32, (8, LANES), 0)
    order = (lane + 1).astype(jnp.float32)
    index = (lane % 16) * 8 + sub
    group = lane // 16
    high = jnp.right_shift(cols, 4)
    low = jnp.bitwise_and(cols, 15)
    left = jnp.concatenate([jnp.where(high == h, 1.0, 0.0) for h in range(8)], axis=0)
    right = jnp.concatenate([jnp.where(low == b, order, 0.0) for b in range(16)], axis=0)
    product = lax.dot_general(
        left.astype(jnp.bfloat16),
        right.astype(jnp.bfloat16),
        (((1,), (1,)), ((), ())),
        preferred_element_type=jnp.float32,
    )
    found = jnp.zeros((8, LANES), jnp.float32)
    for h in range(8):
        found = jnp.where(group == h, lane_take(product[h * 8 : (h + 1) * 8], index), found)
    return found.astype(jnp.int32) - 1


def ice_block(mass, coriolis, start, wind, current):
    pairs, width = mass.shape
    lane = lax.broadcasted_iota(jnp.int32, (pairs, width), 1)
    first, last = lane == 0, lane == width - 1

    def beside(values):
        before = jnp.where(first, 0.0, pltpu.roll(values, 1, 1))
        after = jnp.where(last, 0.0, pltpu.roll(values, width - 1, 1))
        return before + after

    diagonal = mass + drag_coeff + 2.0 * link_coeff
    turning = coriolis * mass
    inverse = 1.0 / (diagonal * diagonal + turning * turning)
    diagonal = diagonal * inverse
    turning = turning * inverse
    east, north = start
    base_east = mass * east + wind[0] + drag_coeff * current[0]
    base_north = mass * north + wind[1] + drag_coeff * current[1]
    for _ in range(ICE_SWEEPS):
        right_east = base_east + link_coeff * beside(east)
        right_north = base_north + link_coeff * beside(north)
        east = diagonal * right_east + turning * right_north
        north = diagonal * right_north - turning * right_east
    return east, north


def around(sizes, body_ref, edge_ref, east_ref, west_ref, south_ref, north_ref, send, recv):
    rows = body_ref.shape[1]
    nz, nm = sizes
    z, m = lax.axis_index("zon"), lax.axis_index("mer")
    top, end = pl.ds(0, ROW_RIM), pl.ds(rows - ROW_RIM, ROW_RIM)
    whole, after, before = pl.ds(0, rows), pl.ds(rows, ROW_RIM), pl.ds(rows + ROW_RIM, ROW_RIM)
    moves = [
        (edge_ref.at[0], east_ref.at[whole], -1, 0),
        (edge_ref.at[1], west_ref.at[whole], 1, 0),
        (body_ref.at[:, top], south_ref, 0, -1),
        (body_ref.at[:, end], north_ref, 0, 1),
        (edge_ref.at[0, top], east_ref.at[after], -1, -1),
        (edge_ref.at[0, end], east_ref.at[before], -1, 1),
        (edge_ref.at[1, top], west_ref.at[after], 1, -1),
        (edge_ref.at[1, end], west_ref.at[before], 1, 1),
    ]
    return [
        pltpu.make_async_remote_copy(
            src_ref=source,
            dst_ref=target,
            send_sem=send.at[i],
            recv_sem=recv.at[i],
            device_id={"zon": lax.rem(z + dz + nz, nz), "mer": lax.rem(m + dm + nm, nm)},
            device_id_type=pl.DeviceIdType.MESH,
        )
        for i, (source, target, dz, dm) in enumerate(moves)
    ]


def pick_group(base, per, turned_ids, parts, cols_ref, values_ref, lanes_ref, group):
    pairs = cols_ref.shape[1]
    lane = lax.broadcasted_iota(jnp.int32, (LANES, LANES), 1)
    turned = jnp.concatenate(
        [
            lane_take(turned_ids, jnp.full((pairs, LANES), base + d, jnp.int32))
            for d in range(per)
        ],
        axis=0,
    )
    lanes_ref[group] = jnp.transpose(turned)[:8]
    pick = jnp.concatenate(
        [
            jnp.where(turned == lane + b * LANES, 1.0, 0.0).astype(jnp.bfloat16)
            for b in range(parts.shape[1] // LANES)
        ],
        axis=1,
    )
    picked = nn_dot(pick, parts[0]) + nn_dot(pick, parts[1]) + nn_dot(pick, parts[2])
    cols = cols_ref[pl.ds(base, per)].reshape(LANES, LANES)
    index = jnp.maximum(cols, 0)
    for c in range(2):
        taken = lane_take(picked[:, c * LANES : (c + 1) * LANES], index)
        taken = jnp.where(cols >= 0, taken, 0.0)
        for d in range(per):
            values_ref[base + d, c] = taken[d * pairs : (d + 1) * pairs]


def put_group(base, per, returned_ref, inverse_ref, lanes_ref, group, count):
    pairs = inverse_ref.shape[1]
    row = lax.broadcasted_iota(jnp.int32, (count, LANES), 0)
    ids = lanes_ref[group]
    put = jnp.where(
        jnp.broadcast_to(ids[:1], (count, LANES)) == row, 1.0, 0.0
    ).astype(jnp.bfloat16)
    inverse = inverse_ref[pl.ds(base, per)].reshape(LANES, LANES)
    index = jnp.maximum(inverse, 0)
    halves = []
    for c in range(2):
        values = jnp.concatenate([returned_ref[base + d, c] for d in range(per)], axis=0)
        halves.append(jnp.where(inverse >= 0, lane_take(values, index), 0.0))
    high, middle, low = split3(jnp.concatenate(halves, axis=1))
    return nn_dot(put, high) + nn_dot(put, middle) + nn_dot(put, low)


def side_tile(k, east_ref, west_ref, known):
    tall = east_ref.shape[0]
    per = LANES // COL_RIM
    slot = lax.broadcasted_iota(jnp.int32, (tall, LANES), 1) // COL_RIM
    at = (k // per) * LANES
    spot = k % per
    east = east_ref[:, at : at + LANES]
    west = west_ref[:, at : at + LANES]
    if spot:
        east = pltpu.roll(east, LANES - spot * COL_RIM, 1)
    if spot != per - 1:
        west = pltpu.roll(west, LANES - (spot + 1) * COL_RIM, 1)
    both = jnp.where(slot == 0, east, jnp.where(slot == per - 1, west, 0.0))
    return jnp.where(known, both, 0.0)


def known_rows(sizes, rows, tall):
    m = lax.axis_index("mer")
    row = lax.broadcasted_iota(jnp.int32, (tall, LANES), 0)
    lower = jnp.where(m == sizes[1] - 1, rows, rows + ROW_RIM)
    upper = jnp.where(m == 0, tall, rows + ROW_RIM)
    return (row < lower) | ((row >= rows + ROW_RIM) & (row >= upper))


def travel_kernel(
    sizes,
    current_hbm, blocks_hbm, cols_hbm, mass_hbm, coriolis_hbm, start_hbm, wind_hbm,
    sea_hbm, forcing_hbm, weights_hbm, excess_hbm, mask_hbm,
    velocity_ref, halves_ref, stress_ref, late_east, late_west, late_south, late_north,
    current_ref, blocks_ref, square, cols_ref, mass_ref, coriolis_ref, start_ref, wind_ref,
    sea_ref, forcing_ref, weights_ref, excess_ref, mask_ref,
    parts, lanes_ref, values_ref, arrived, drag, returned_ref, inverse_ref, total,
    body_ref, edge, east_ref, west_ref, south_ref, north_ref, field, stress_edge,
    loads, send_out, recv_out, send_back, recv_back, send_rim, recv_rim, send_late, recv_late,
):
    nz, nm = sizes
    count = nz * nm
    z, m = lax.axis_index("zon"), lax.axis_index("mer")
    me = z * nm + m
    _, rows, width = current_ref.shape
    tiles = width // LANES
    devices, pairs, _ = cols_ref.shape
    per = LANES // pairs
    span = per // nm
    groups = count // per
    mine = lax.div(z, span)

    def group_of(i):
        return lax.rem(mine + groups // 2 + lax.div(i + 1, 2) * (1 - 2 * lax.rem(i, 2)), groups)

    def group_from(i):
        return lax.rem(
            mine + groups + groups // 2 - lax.div(i + 1, 2) * (1 - 2 * lax.rem(i, 2)), groups
        )

    def member(group, k):
        inner = lax.rem(k, per)
        a = lax.rem(lax.rem(z, span) + span - 1 - lax.div(inner, nm), span)
        return group * span + a, lax.rem(m + nm - 1 - lax.rem(inner, nm), nm)

    def member_from(group, k):
        inner = lax.rem(k, per)
        a = lax.rem(lax.rem(z, span) + 1 + lax.div(inner, nm), span)
        return group * span + a, lax.rem(m + 1 + lax.rem(inner, nm), nm)

    def ahead(k):
        return member(group_of(lax.div(k, per)), k)

    def behind(k):
        return member_from(group_from(lax.div(k, per)), k)

    def out_copy(k):
        pz, pm = ahead(k)
        return pltpu.make_async_remote_copy(
            src_ref=values_ref.at[pz * nm + pm],
            dst_ref=arrived.at[me],
            send_sem=send_out.at[k],
            recv_sem=recv_out.at[k],
            device_id={"zon": pz, "mer": pm},
            device_id_type=pl.DeviceIdType.MESH,
        )

    def back_copy(k):
        pz, pm = behind(k)
        return pltpu.make_async_remote_copy(
            src_ref=drag.at[k],
            dst_ref=returned_ref.at[me],
            send_sem=send_back.at[k],
            recv_sem=recv_back.at[k],
            device_id={"zon": pz, "mer": pm},
            device_id_type=pl.DeviceIdType.MESH,
        )

    barrier = pltpu.get_barrier_semaphore()

    def greet(k, carry):
        pz, pm = ahead(k)
        pl.semaphore_signal(
            barrier,
            inc=1,
            device_id={"zon": pz, "mer": pm},
            device_id_type=pl.DeviceIdType.MESH,
        )
        return carry

    copies = [
        pltpu.make_async_copy(source, target, loads.at[i])
        for i, (source, target) in enumerate(
            [
                (current_hbm, current_ref),
                (blocks_hbm.at[0], blocks_ref),
                (cols_hbm.at[0], cols_ref),
                (mass_hbm.at[0], mass_ref),
                (coriolis_hbm.at[0], coriolis_ref),
                (start_hbm.at[:, 0], start_ref),
                (wind_hbm.at[:, 0], wind_ref),
                (weights_hbm, weights_ref),
                (sea_hbm, sea_ref),
                (forcing_hbm, forcing_ref),
                (excess_hbm, excess_ref),
                (mask_hbm, mask_ref),
            ]
        )
    ]
    for copy in copies:
        copy.start()
    lax.fori_loop(0, count - 1, greet, 0)

    copies[0].wait()
    for j in range(tiles):
        for c in range(2):
            for k, part in enumerate(split3(current_ref[c, :, j * LANES : (j + 1) * LANES])):
                parts[k, j * rows : (j + 1) * rows, c * LANES : (c + 1) * LANES] = part
    copies[1].wait()
    square[:devices, :pairs] = block_rows(blocks_ref[...], tiles, rows)
    turned_ids = jnp.transpose(square[...])[:pairs]
    copies[2].wait()

    def pick(i, carry):
        group = group_of(i)
        pick_group(group * per, per, turned_ids, parts, cols_ref, values_ref, lanes_ref, group)
        return carry

    lax.fori_loop(0, groups, pick, 0)
    pl.semaphore_wait(barrier, count - 1)

    def launch(k, carry):
        out_copy(k).start()
        return carry

    lax.fori_loop(0, count - 1, launch, 0)

    for copy in copies[3:]:
        copy.wait()
    prepare_kernel(sea_ref, forcing_ref, weights_ref, excess_ref, mask_ref, body_ref, edge)

    def ice(at, from_ref):
        current = (from_ref[at, 0], from_ref[at, 1])
        east, north = ice_block(
            mass_ref[at],
            coriolis_ref[at],
            (start_ref[0, at], start_ref[1, at]),
            (wind_ref[0, at], wind_ref[1, at]),
            current,
        )
        velocity_ref[0, at] = east
        velocity_ref[1, at] = north
        return drag_coeff * (east - current[0]), drag_coeff * (north - current[1])

    def invert(k):
        for r in range(0, pairs, 8):
            inverse_ref[k, r : r + 8] = inverse_rows(cols_ref[k, r : r + 8])

    own_east, own_north = ice(me, values_ref)
    invert(count - 1)
    returned_ref[me, 0] = own_east
    returned_ref[me, 1] = own_north

    rim = around(
        sizes, body_ref, edge, east_ref, west_ref, south_ref, north_ref, send_rim, recv_rim
    )
    for copy in rim:
        copy.start()

    def step(k, carry):
        out_copy(k).wait_recv()
        pz, pm = behind(k)
        east, north = ice(pz * nm + pm, arrived)
        drag[k, 0] = east
        drag[k, 1] = north
        invert(k)

        @pl.when(k > 0)
        def _():
            back_copy(k - 1).start()

        return carry

    lax.fori_loop(0, count - 1, step, 0)
    back_copy(count - 2).start()

    for copy in rim:
        copy.wait()
    tall, wide = rows + 2 * ROW_RIM, width + LANES
    half = tall // 2
    wide_tiles = wide // LANES
    known = known_rows(sizes, rows, tall)
    has_south, has_north = m < nm - 1, m > 0
    for k in range(body_ref.shape[0]):
        for t in range(tiles):
            part = slice(t * LANES, (t + 1) * LANES)
            field[t, :rows] = body_ref[k, :, part]
            field[t, rows : rows + ROW_RIM] = jnp.where(has_south, south_ref[k, :, part], 0.0)
            field[t, rows + ROW_RIM :] = jnp.where(has_north, north_ref[k, :, part], 0.0)
        field[tiles] = side_tile(k, east_ref, west_ref, known)
        for t in range(wide_tiles):
            part = slice(t * LANES, (t + 1) * LANES)
            halves_ref[k, 0, :, part] = field[t, pl.ds(0, half, stride=2), :]
            halves_ref[k, 1, :, part] = field[t, pl.ds(1, half, stride=2), :]

    def collect(i, carry):
        group = group_of(i)

        def arrive(k, inner):
            back_copy(k).wait_recv()
            return inner

        lax.fori_loop(i * per, jnp.minimum(i * per + per, count - 1), arrive, 0)
        added = put_group(
            group * per, per, returned_ref, inverse_ref, lanes_ref, group, rows * tiles
        )

        @pl.when(i == 0)
        def _():
            total[...] = added

        @pl.when(i > 0)
        def _():
            total[...] += added

        return carry

    lax.fori_loop(0, groups, collect, 0)
    for c in range(2):
        for j in range(tiles):
            stress_ref[c, :, j * LANES : (j + 1) * LANES] = total[
                j * rows : (j + 1) * rows, c * LANES : (c + 1) * LANES
            ]
    pack_edges([stress_ref.at[0], stress_ref.at[1]], stress_edge)
    late = around(
        sizes, stress_ref, stress_edge, late_east, late_west, late_south, late_north,
        send_late, recv_late,
    )
    for copy in late:
        copy.start()

    def finish(k, carry):
        out_copy(k).wait_send()
        back_copy(k).wait_send()
        return carry

    lax.fori_loop(0, count - 1, finish, 0)
    for copy in late:
        copy.wait()


def pack_edges(refs, edge_ref):
    rows, width = refs[0].shape
    per = LANES // COL_RIM
    slot = lax.broadcasted_iota(jnp.int32, (rows, LANES), 1) // COL_RIM
    for start in range(0, len(refs), per):
        tile = start // per
        first = jnp.zeros((rows, LANES), jnp.float32)
        last = first
        for k, ref in enumerate(refs[start : start + per]):
            head = ref[:, :LANES]
            tail = ref[:, width - LANES :]
            if k:
                head = pltpu.roll(head, k * COL_RIM, 1)
            if (k + 1) * COL_RIM != LANES:
                tail = pltpu.roll(tail, (k + 1) * COL_RIM, 1)
            first = jnp.where(slot == k, head, first)
            last = jnp.where(slot == k, tail, last)
        edge_ref[0, :, tile * LANES : (tile + 1) * LANES] = first
        edge_ref[1, :, tile * LANES : (tile + 1) * LANES] = last


def prepare_kernel(sea_ref, forcing_ref, weights_ref, excess_ref, mask_ref, out_ref, edge_ref):
    total = weights_ref[0]
    for k in range(1, 8):
        total = total + weights_ref[k]
    ocean = mask_ref[...] > 0
    inverse = jnp.where(ocean, 1.0 / ((1.0 + excess_ref[...]) * total), 0.0)
    for k in range(8):
        out_ref[k] = weights_ref[k] * inverse
    out_ref[8] = inverse
    out_ref[9] = jnp.where(ocean, sea_ref[...], 0.0)
    out_ref[10] = forcing_ref[...]
    pack_edges([out_ref.at[k] for k in range(out_ref.shape[0])], edge_ref)


def sweep_kernel(
    sizes,
    halves_ref, stress_ref, late_east, late_west, late_south, late_north, velocity_ref,
    out_ref, velocity_hbm,
    wide_ref, tile_ref, even_ref, odd_ref, write,
):
    _, rows, width = stress_ref.shape
    tall, wide = rows + 2 * ROW_RIM, width + LANES
    half = tall // 2
    tiles = wide // LANES
    write_velocity = pltpu.make_async_copy(velocity_ref, velocity_hbm, write)
    write_velocity.start()
    m = lax.axis_index("mer")
    has_south, has_north = m < sizes[1] - 1, m > 0
    known = known_rows(sizes, rows, tall)
    for c in range(2):
        wide_ref[c, :rows, :width] = stress_ref[c]
        wide_ref[c, rows : rows + ROW_RIM, :width] = jnp.where(has_south, late_south[c], 0.0)
        wide_ref[c, rows + ROW_RIM :, :width] = jnp.where(has_north, late_north[c], 0.0)
        wide_ref[c, :, width:] = side_tile(c, late_east, late_west, known)
    east_stress = wide_ref[0]
    north_stress = wide_ref[1]
    change = (
        pltpu.roll(north_stress, wide - 1, 1)
        - pltpu.roll(north_stress, 1, 1)
        - pltpu.roll(east_stress, tall - 1, 0)
        + pltpu.roll(east_stress, 1, 0)
    )
    for t in range(tiles):
        tile_ref[t] = change[:, t * LANES : (t + 1) * LANES]

    def take(k, which):
        return halves_ref[k, which]

    for which in range(2):
        rows_of = pl.ds(which, half, stride=2)
        for t in range(tiles):
            part = slice(t * LANES, (t + 1) * LANES)
            wide_ref[which, :half, part] = (
                halves_ref[10, which, :, part] + tile_ref[t, rows_of, :]
            ) * halves_ref[8, which, :, part]

    column_odd = lax.broadcasted_iota(jnp.int32, (half, wide), 1) % 2
    even_ref[...] = take(9, 0)
    odd_ref[...] = take(9, 1)

    def phase(own_ref, other_ref, odd, colours):
        base = wide_ref[odd, :half]
        other = other_ref[...]
        if odd:
            above, below = other, pltpu.roll(other, half - 1, 0)
        else:
            above, below = pltpu.roll(other, 1, 0), other
        base = base + take(2, odd) * below + take(3, odd) * above
        base = base + take(4, odd) * pltpu.roll(below, wide - 1, 1)
        base = base + take(5, odd) * pltpu.roll(below, 1, 1)
        base = base + take(6, odd) * pltpu.roll(above, wide - 1, 1)
        base = base + take(7, odd) * pltpu.roll(above, 1, 1)
        own = own_ref[...]
        for parity in colours:
            new = base + take(0, odd) * pltpu.roll(own, wide - 1, 1)
            new = new + take(1, odd) * pltpu.roll(own, 1, 1)
            own = jnp.where(column_odd == parity, new, own)
        own_ref[...] = own

    runs = [(0, [0, 1])]
    for _ in range(SWEEPS):
        runs += [(1, [0, 1, 0]), (0, [1, 0, 1])]
    runs[-1] = (0, [1, 0])
    for odd, colours in runs:
        if odd:
            phase(odd_ref, even_ref, 1, colours)
        else:
            phase(even_ref, odd_ref, 0, colours)
    for t in range(tiles - 1):
        part = slice(t * LANES, (t + 1) * LANES)
        tile_ref[t, pl.ds(0, rows // 2, stride=2), :] = even_ref[: rows // 2, part]
        tile_ref[t, pl.ds(1, rows // 2, stride=2), :] = odd_ref[: rows // 2, part]
        out_ref[:, part] = tile_ref[t, :rows, :]
    write_velocity.wait()


def local(
    sea_level,
    forcing,
    link_weights,
    excess,
    ocean_mask,
    current,
    intersection_block,
    intersection_cols,
    ice_mass,
    coriolis,
    ice_start,
    wind_stress,
):
    rows, width = sea_level.shape
    _, devices, pairs, block = intersection_cols.shape
    slots = devices * pairs
    tiles = width // LANES
    f32 = jnp.float32
    ice_shape = (devices, pairs, block)
    slot_bytes = slots * block * 4
    sizes = (lax.axis_size("zon"), lax.axis_size("mer"))
    arrays = 11
    tall, wide = rows + 2 * ROW_RIM, width + LANES
    edge_width = -(-arrays * COL_RIM // LANES) * LANES
    dma = pltpu.SemaphoreType.DMA
    shape = jax.ShapeDtypeStruct
    stay = functools.partial(pltpu.with_memory_space_constraint, memory_space=pltpu.HBM)
    velocity, halves, *late = pl.pallas_call(
        functools.partial(travel_kernel, sizes),
        out_shape=(
            shape((2,) + ice_shape, f32),
            shape((arrays, 2, tall // 2, wide), f32),
            shape((2, rows, width), f32),
            shape((tall, LANES), f32),
            shape((tall, LANES), f32),
            shape((2, ROW_RIM, width), f32),
            shape((2, ROW_RIM, width), f32),
        ),
        in_specs=[HBM] * 12,
        out_specs=(VM,) * 7,
        scratch_shapes=[
            pltpu.VMEM((2, rows, width), f32),
            pltpu.VMEM((devices, pairs), jnp.int32),
            pltpu.VMEM((LANES, LANES), jnp.int32),
            pltpu.VMEM(ice_shape, jnp.int32),
            pltpu.VMEM(ice_shape, f32),
            pltpu.VMEM(ice_shape, f32),
            pltpu.VMEM((2,) + ice_shape, f32),
            pltpu.VMEM((2,) + ice_shape, f32),
            pltpu.VMEM((rows, width), f32),
            pltpu.VMEM((rows, width), f32),
            pltpu.VMEM((8, rows, width), f32),
            pltpu.VMEM((rows, width), f32),
            pltpu.VMEM((rows, width), jnp.int32),
            pltpu.VMEM((3, rows * tiles, 2 * LANES), jnp.bfloat16),
            pltpu.VMEM((slots // LANES, 8, LANES), jnp.int32),
            pltpu.VMEM((devices, 2, pairs, block), f32),
            pltpu.VMEM((devices, 2, pairs, block), f32),
            pltpu.VMEM((devices, 2, pairs, block), f32),
            pltpu.VMEM((devices, 2, pairs, block), f32),
            pltpu.VMEM(ice_shape, jnp.int32),
            pltpu.VMEM((rows * tiles, 2 * LANES), f32),
            pltpu.VMEM((arrays, rows, width), f32),
            pltpu.VMEM((2, rows, edge_width), f32),
            pltpu.VMEM((tall, edge_width), f32),
            pltpu.VMEM((tall, edge_width), f32),
            pltpu.VMEM((arrays, ROW_RIM, width), f32),
            pltpu.VMEM((arrays, ROW_RIM, width), f32),
            pltpu.VMEM((wide // LANES, tall, LANES), f32),
            pltpu.VMEM((2, rows, LANES), f32),
            dma((12,)),
            dma((devices,)),
            dma((devices,)),
            dma((devices,)),
            dma((devices,)),
            dma((8,)),
            dma((8,)),
            dma((8,)),
            dma((8,)),
        ],
        compiler_params=pltpu.CompilerParams(
            vmem_limit_bytes=TRAVEL_VMEM, collective_id=0, has_side_effects=True
        ),
        cost_estimate=cost(slots * block * 4096, 16 * slot_bytes),
        name="travel",
    )(
        stay(current),
        stay(intersection_block),
        stay(intersection_cols),
        stay(ice_mass),
        stay(coriolis),
        stay(ice_start),
        stay(wind_stress),
        stay(sea_level),
        stay(forcing),
        stay(link_weights),
        stay(excess),
        stay(ocean_mask),
    )
    surface, velocity = pl.pallas_call(
        functools.partial(sweep_kernel, sizes),
        out_shape=(shape((rows, width), f32), shape((2,) + ice_shape, f32)),
        in_specs=[VM] * 7,
        out_specs=(VM, HBM),
        scratch_shapes=[
            pltpu.VMEM((2, tall, wide), f32),
            pltpu.VMEM((wide // LANES, tall, LANES), f32),
            pltpu.VMEM((tall // 2, wide), f32),
            pltpu.VMEM((tall // 2, wide), f32),
            dma,
        ],
        compiler_params=pltpu.CompilerParams(vmem_limit_bytes=SWEEP_VMEM),
        cost_estimate=cost(rows * width * 200, rows * width * 64),
        name="sweep",
    )(halves, *late, velocity)
    return (surface, velocity.reshape((2, 1) + ice_shape))


def solution(mesh):
    return jax.shard_map(
        local,
        mesh=mesh,
        in_specs=(
            P("mer", "zon"),
            P("mer", "zon"),
            P(None, "mer", "zon"),
            P("mer", "zon"),
            P("mer", "zon"),
            P(None, "mer", "zon"),
            P(("zon", "mer"), None, None),
            P(("zon", "mer"), None, None, None),
            P(("zon", "mer"), None, None, None),
            P(("zon", "mer"), None, None, None),
            P(None, ("zon", "mer"), None, None, None),
            P(None, ("zon", "mer"), None, None, None),
        ),
        out_specs=(P("mer", "zon"), P(None, ("zon", "mer"), None, None, None)),
        check_vma=False,
    )
```

```python
import functools

import jax
import jax.numpy as jnp
from jax import lax
from jax.experimental import pallas as pl
from jax.experimental.pallas import tpu as pltpu
from jax.sharding import PartitionSpec as P

SWEEPS = 2
ICE_SWEEPS = 3
ROW_RIM = 8
COL_RIM = 16
LANES = 128
EAST_COLS = 11
WEST_COLS = 12
EXTRA_COLS = 8
FIELD = 9

drag_coeff = 1.0
link_coeff = 0.5
VM = pl.BlockSpec(memory_space=pltpu.VMEM)
HBM = pl.BlockSpec(memory_space=pltpu.HBM)
TRAVEL_VMEM = 40 * 1024 * 1024
SWEEP_VMEM = 16 * 1024 * 1024


def cost(flops, nbytes):
    return pl.CostEstimate(flops=flops, bytes_accessed=nbytes, transcendentals=0)


def lane_take(values, index):
    return jnp.take_along_axis(values, index, axis=1, mode="promise_in_bounds")


def split3(values):
    high = values.astype(jnp.bfloat16)
    rest = values - high.astype(jnp.float32)
    middle = rest.astype(jnp.bfloat16)
    low = (rest - middle.astype(jnp.float32)).astype(jnp.bfloat16)
    return high, middle, low


def nn_dot(a, b):
    return lax.dot_general(a, b, (((1,), (0,)), ((), ())), preferred_element_type=jnp.float32)


def block_rows(blocks, tiles, rows):
    safe = jnp.maximum(blocks, 0)
    return jnp.where(blocks >= 0, (safe % tiles) * rows + safe // tiles, -1)


def inverse_rows(cols):
    lane = lax.broadcasted_iota(jnp.int32, (8, LANES), 1)
    sub = lax.broadcasted_iota(jnp.int32, (8, LANES), 0)
    order = (lane + 1).astype(jnp.float32)
    index = (lane % 16) * 8 + sub
    group = lane // 16
    high = jnp.right_shift(cols, 4)
    low = jnp.bitwise_and(cols, 15)
    left = jnp.concatenate([jnp.where(high == h, 1.0, 0.0) for h in range(8)], axis=0)
    right = jnp.concatenate([jnp.where(low == b, order, 0.0) for b in range(16)], axis=0)
    product = lax.dot_general(
        left.astype(jnp.bfloat16),
        right.astype(jnp.bfloat16),
        (((1,), (1,)), ((), ())),
        preferred_element_type=jnp.float32,
    )
    found = jnp.zeros((8, LANES), jnp.float32)
    for h in range(8):
        found = jnp.where(group == h, lane_take(product[h * 8 : (h + 1) * 8], index), found)
    return found.astype(jnp.int32) - 1


def ice_block(mass, coriolis, start, wind, current):
    pairs, width = mass.shape
    lane = lax.broadcasted_iota(jnp.int32, (pairs, width), 1)
    first, last = lane == 0, lane == width - 1

    def beside(values):
        before = jnp.where(first, 0.0, pltpu.roll(values, 1, 1))
        after = jnp.where(last, 0.0, pltpu.roll(values, width - 1, 1))
        return before + after

    diagonal = mass + drag_coeff + 2.0 * link_coeff
    turning = coriolis * mass
    inverse = 1.0 / (diagonal * diagonal + turning * turning)
    diagonal = diagonal * inverse
    turning = turning * inverse
    east, north = start
    base_east = mass * east + wind[0] + drag_coeff * current[0]
    base_north = mass * north + wind[1] + drag_coeff * current[1]
    for _ in range(ICE_SWEEPS):
        right_east = base_east + link_coeff * beside(east)
        right_north = base_north + link_coeff * beside(north)
        east = diagonal * right_east + turning * right_north
        north = diagonal * right_north - turning * right_east
    return east, north


def around(sizes, body_ref, edge_ref, east_ref, west_ref, south_ref, north_ref, send, recv):
    rows = body_ref.shape[1]
    top, end = pl.ds(0, ROW_RIM), pl.ds(rows - ROW_RIM, ROW_RIM)
    whole, after, before = pl.ds(0, rows), pl.ds(rows, ROW_RIM), pl.ds(rows + ROW_RIM, ROW_RIM)
    moves = [
        (edge_ref.at[0], east_ref.at[whole], -1, 0),
        (edge_ref.at[1], west_ref.at[whole], 1, 0),
        (body_ref.at[:, top], south_ref, 0, -1),
        (body_ref.at[:, end], north_ref, 0, 1),
        (edge_ref.at[0, top], east_ref.at[after], -1, -1),
        (edge_ref.at[0, end], east_ref.at[before], -1, 1),
        (edge_ref.at[1, top], west_ref.at[after], 1, -1),
        (edge_ref.at[1, end], west_ref.at[before], 1, 1),
    ]
    return neighbour_copies(sizes, moves, send, recv)


def neighbour_copies(sizes, moves, send, recv):
    nz, nm = sizes
    z, m = lax.axis_index("zon"), lax.axis_index("mer")
    return [
        pltpu.make_async_remote_copy(
            src_ref=source,
            dst_ref=target,
            send_sem=send.at[i],
            recv_sem=recv.at[i],
            device_id={"zon": lax.rem(z + dz + nz, nz), "mer": lax.rem(m + dm + nm, nm)},
            device_id_type=pl.DeviceIdType.MESH,
        )
        for i, (source, target, dz, dm) in enumerate(moves)
    ]


def pick_group(base, per, turned_ids, parts, cols_ref, values_ref, lanes_ref, group):
    pairs = cols_ref.shape[1]
    lane = lax.broadcasted_iota(jnp.int32, (LANES, LANES), 1)
    turned = jnp.concatenate(
        [
            lane_take(turned_ids, jnp.full((pairs, LANES), base + d, jnp.int32))
            for d in range(per)
        ],
        axis=0,
    )
    lanes_ref[group] = jnp.transpose(turned)[:8]
    pick = jnp.concatenate(
        [
            jnp.where(turned == lane + b * LANES, 1.0, 0.0).astype(jnp.bfloat16)
            for b in range(parts.shape[1] // LANES)
        ],
        axis=1,
    )
    picked = nn_dot(pick, parts[0]) + nn_dot(pick, parts[1]) + nn_dot(pick, parts[2])
    cols = cols_ref[pl.ds(base, per)].reshape(LANES, LANES)
    index = jnp.maximum(cols, 0)
    for c in range(2):
        taken = lane_take(picked[:, c * LANES : (c + 1) * LANES], index)
        taken = jnp.where(cols >= 0, taken, 0.0)
        for d in range(per):
            values_ref[base + d, c] = taken[d * pairs : (d + 1) * pairs]


def put_group(base, per, returned_ref, inverse_ref, lanes_ref, group, count):
    pairs = inverse_ref.shape[1]
    row = lax.broadcasted_iota(jnp.int32, (count, LANES), 0)
    ids = lanes_ref[group]
    put = jnp.where(
        jnp.broadcast_to(ids[:1], (count, LANES)) == row, 1.0, 0.0
    ).astype(jnp.bfloat16)
    inverse = inverse_ref[pl.ds(base, per)].reshape(LANES, LANES)
    index = jnp.maximum(inverse, 0)
    halves = []
    for c in range(2):
        values = jnp.concatenate([returned_ref[base + d, c] for d in range(per)], axis=0)
        halves.append(jnp.where(inverse >= 0, lane_take(values, index), 0.0))
    high, middle, low = split3(jnp.concatenate(halves, axis=1))
    return nn_dot(put, high) + nn_dot(put, middle) + nn_dot(put, low)


def side_tile(k, east_ref, west_ref, known):
    tall = east_ref.shape[0]
    per = LANES // COL_RIM
    slot = lax.broadcasted_iota(jnp.int32, (tall, LANES), 1) // COL_RIM
    at = (k // per) * LANES
    spot = k % per
    east = east_ref[:, at : at + LANES]
    west = west_ref[:, at : at + LANES]
    if spot:
        east = pltpu.roll(east, LANES - spot * COL_RIM, 1)
    if spot != per - 1:
        west = pltpu.roll(west, LANES - (spot + 1) * COL_RIM, 1)
    both = jnp.where(slot == 0, east, jnp.where(slot == per - 1, west, 0.0))
    return jnp.where(known, both, 0.0)


def known_rows(sizes, rows, tall):
    m = lax.axis_index("mer")
    row = lax.broadcasted_iota(jnp.int32, (tall, LANES), 0)
    lower = jnp.where(m == sizes[1] - 1, rows, rows + ROW_RIM)
    upper = jnp.where(m == 0, tall, rows + ROW_RIM)
    return (row < lower) | ((row >= rows + ROW_RIM) & (row >= upper))


def rim_lanes(arrays):
    order = [k for k in range(arrays) if k != FIELD] + [FIELD]
    return [(k, i * EAST_COLS, i * WEST_COLS) for i, k in enumerate(order)]


def pack_rims(body_ref, edge_ref):
    arrays, rows, width = body_ref.shape
    lane = lax.broadcasted_iota(jnp.int32, (rows, LANES), 1)
    first = jnp.zeros((rows, LANES), jnp.float32)
    last = first
    for k, east, west in rim_lanes(arrays):
        head = body_ref[k, :, :LANES]
        tail = body_ref[k, :, width - LANES :]
        if east:
            head = pltpu.roll(head, east, 1)
        first = jnp.where(lane >= east, head, first)
        if k == FIELD:
            last = jnp.where(lane >= west, tail, last)
        else:
            tail = pltpu.roll(tail, west + WEST_COLS, 1)
            last = jnp.where((lane >= west) & (lane < west + WEST_COLS), tail, last)
    edge_ref[0, :rows] = first
    edge_ref[1, :rows] = last
    near = lane[:ROW_RIM]
    extra = jnp.zeros((ROW_RIM, LANES), jnp.float32)
    for g in range(rows // ROW_RIM):
        piece = body_ref[FIELD, g * ROW_RIM : (g + 1) * ROW_RIM, width - LANES :]
        at = g * EXTRA_COLS
        shift = (at + COL_RIM) % LANES
        if shift:
            piece = pltpu.roll(piece, shift, 1)
        extra = jnp.where((near >= at) & (near < at + EXTRA_COLS), piece, extra)
    edge_ref[1, rows : rows + ROW_RIM] = extra
    edge_ref[0, rows : rows + ROW_RIM] = extra


def rim_moves(sizes, body_ref, edge_ref, east_ref, west_ref, south_ref, north_ref, send, recv):
    rows = body_ref.shape[1]
    end = rows - ROW_RIM

    def part(at, count=ROW_RIM):
        return pl.ds(at, count)

    return neighbour_copies(
        sizes,
        [
            (edge_ref.at[0, part(0, rows)], east_ref.at[part(0, rows)], -1, 0),
            (edge_ref.at[1], west_ref.at[part(0, rows + ROW_RIM)], 1, 0),
            (body_ref.at[:, part(0)], south_ref, 0, -1),
            (body_ref.at[:, part(end)], north_ref, 0, 1),
            (edge_ref.at[0, part(0)], east_ref.at[part(rows)], -1, -1),
            (edge_ref.at[0, part(end)], east_ref.at[part(rows + ROW_RIM)], -1, 1),
            (edge_ref.at[1, part(0)], west_ref.at[part(rows + ROW_RIM)], 1, -1),
            (edge_ref.at[1, part(end)], west_ref.at[part(rows + 2 * ROW_RIM)], 1, 1),
            (edge_ref.at[1, part(rows)], west_ref.at[part(rows + 3 * ROW_RIM)], 1, -1),
            (edge_ref.at[1, part(rows)], west_ref.at[part(rows + 4 * ROW_RIM)], 1, 1),
        ],
        send,
        recv,
    )


def extra_columns(west_ref, rows):
    pieces = []
    for g in range(rows // ROW_RIM):
        shift = (2 * LANES - COL_RIM - g * EXTRA_COLS) % LANES
        piece = west_ref[rows : rows + ROW_RIM]
        pieces.append(pltpu.roll(piece, shift, 1) if shift else piece)
    south = west_ref[rows + 3 * ROW_RIM : rows + 4 * ROW_RIM]
    north = west_ref[rows + 4 * ROW_RIM : rows + 5 * ROW_RIM]
    pieces.append(pltpu.roll(south, LANES - COL_RIM, 1))
    last = (2 * LANES - COL_RIM - (rows // ROW_RIM - 1) * EXTRA_COLS) % LANES
    pieces.append(pltpu.roll(north, last, 1) if last else north)
    return jnp.concatenate(pieces, axis=0)


def rim_tile(k, east_at, west_at, east_ref, west_ref, extra, rows, known):
    tall = rows + 2 * ROW_RIM
    lane = lax.broadcasted_iota(jnp.int32, (tall, LANES), 1)
    east = east_ref[...]
    west = jnp.concatenate(
        [west_ref[:rows], west_ref[rows + ROW_RIM : rows + 3 * ROW_RIM]], axis=0
    )
    if east_at:
        east = pltpu.roll(east, LANES - east_at, 1)
    if k == FIELD:
        kept, near = EAST_COLS + 1, LANES - (LANES - west_at)
        west = jnp.where(lane >= near, west, extra)
        first = LANES - COL_RIM
    else:
        kept, first = EAST_COLS, LANES - WEST_COLS
        west = pltpu.roll(west, LANES - west_at - WEST_COLS, 1)
    both = jnp.where(lane < kept, east, jnp.where(lane >= first, west, 0.0))
    return jnp.where(known, both, 0.0)


def travel_kernel(
    sizes,
    current_hbm, blocks_hbm, cols_hbm, mass_hbm, coriolis_hbm, start_hbm, wind_hbm,
    sea_hbm, forcing_hbm, weights_hbm, excess_hbm, mask_hbm,
    velocity_ref, halves_ref, stress_ref, late_east, late_west, late_south, late_north,
    current_ref, blocks_ref, square, cols_ref, mass_ref, coriolis_ref, start_ref, wind_ref,
    sea_ref, forcing_ref, weights_ref, excess_ref, mask_ref,
    parts, lanes_ref, values_ref, arrived, drag, returned_ref, inverse_ref, total,
    body_ref, edge, east_ref, west_ref, south_ref, north_ref, field, stress_edge,
    loads, send_out, recv_out, send_back, recv_back, send_rim, recv_rim, send_late, recv_late,
):
    nz, nm = sizes
    count = nz * nm
    z, m = lax.axis_index("zon"), lax.axis_index("mer")
    me = z * nm + m
    _, rows, width = current_ref.shape
    tiles = width // LANES
    devices, pairs, _ = cols_ref.shape
    per = LANES // pairs
    span = per // nm
    groups = count // per
    mine = lax.div(z, span)

    def group_of(i):
        return lax.rem(mine + groups // 2 + lax.div(i + 1, 2) * (1 - 2 * lax.rem(i, 2)), groups)

    def group_from(i):
        return lax.rem(
            mine + groups + groups // 2 - lax.div(i + 1, 2) * (1 - 2 * lax.rem(i, 2)), groups
        )

    def member(group, k):
        inner = lax.rem(k, per)
        a = lax.rem(lax.rem(z, span) + span - 1 - lax.div(inner, nm), span)
        return group * span + a, lax.rem(m + nm - 1 - lax.rem(inner, nm), nm)

    def member_from(group, k):
        inner = lax.rem(k, per)
        a = lax.rem(lax.rem(z, span) + 1 + lax.div(inner, nm), span)
        return group * span + a, lax.rem(m + 1 + lax.rem(inner, nm), nm)

    def ahead(k):
        return member(group_of(lax.div(k, per)), k)

    def behind(k):
        return member_from(group_from(lax.div(k, per)), k)

    def out_copy(k):
        pz, pm = ahead(k)
        return pltpu.make_async_remote_copy(
            src_ref=values_ref.at[pz * nm + pm],
            dst_ref=arrived.at[me],
            send_sem=send_out.at[k],
            recv_sem=recv_out.at[k],
            device_id={"zon": pz, "mer": pm},
            device_id_type=pl.DeviceIdType.MESH,
        )

    def back_copy(k):
        pz, pm = behind(k)
        return pltpu.make_async_remote_copy(
            src_ref=drag.at[k],
            dst_ref=returned_ref.at[me],
            send_sem=send_back.at[k],
            recv_sem=recv_back.at[k],
            device_id={"zon": pz, "mer": pm},
            device_id_type=pl.DeviceIdType.MESH,
        )

    barrier = pltpu.get_barrier_semaphore()

    def greet(k, carry):
        pz, pm = ahead(k)
        pl.semaphore_signal(
            barrier,
            inc=1,
            device_id={"zon": pz, "mer": pm},
            device_id_type=pl.DeviceIdType.MESH,
        )
        return carry

    copies = [
        pltpu.make_async_copy(source, target, loads.at[i])
        for i, (source, target) in enumerate(
            [
                (current_hbm, current_ref),
                (blocks_hbm.at[0], blocks_ref),
                (cols_hbm.at[0], cols_ref),
                (mass_hbm.at[0], mass_ref),
                (coriolis_hbm.at[0], coriolis_ref),
                (start_hbm.at[:, 0], start_ref),
                (wind_hbm.at[:, 0], wind_ref),
                (weights_hbm, weights_ref),
                (sea_hbm, sea_ref),
                (forcing_hbm, forcing_ref),
                (excess_hbm, excess_ref),
                (mask_hbm, mask_ref),
            ]
        )
    ]
    for copy in copies:
        copy.start()
    lax.fori_loop(0, count - 1, greet, 0)

    copies[0].wait()
    for j in range(tiles):
        for c in range(2):
            for k, part in enumerate(split3(current_ref[c, :, j * LANES : (j + 1) * LANES])):
                parts[k, j * rows : (j + 1) * rows, c * LANES : (c + 1) * LANES] = part
    copies[1].wait()
    square[:devices, :pairs] = block_rows(blocks_ref[...], tiles, rows)
    turned_ids = jnp.transpose(square[...])[:pairs]
    copies[2].wait()

    def pick(i, carry):
        group = group_of(i)
        pick_group(group * per, per, turned_ids, parts, cols_ref, values_ref, lanes_ref, group)
        return carry

    def launch(k, carry):
        out_copy(k).start()
        return carry

    first = min(2, groups)
    lax.fori_loop(0, first, pick, 0)
    pl.semaphore_wait(barrier, count - 1)

    def pick_and_launch(i, carry):
        lax.fori_loop((i - first) * per, (i - first + 1) * per, launch, 0)
        return pick(i, carry)

    lax.fori_loop(first, groups, pick_and_launch, 0)
    lax.fori_loop((groups - first) * per, count - 1, launch, 0)

    for copy in copies[3:]:
        copy.wait()
    prepare_kernel(sea_ref, forcing_ref, weights_ref, excess_ref, mask_ref, body_ref, edge)

    def ice(at, from_ref):
        current = (from_ref[at, 0], from_ref[at, 1])
        east, north = ice_block(
            mass_ref[at],
            coriolis_ref[at],
            (start_ref[0, at], start_ref[1, at]),
            (wind_ref[0, at], wind_ref[1, at]),
            current,
        )
        velocity_ref[0, at] = east
        velocity_ref[1, at] = north
        return drag_coeff * (east - current[0]), drag_coeff * (north - current[1])

    def invert(k):
        for r in range(0, pairs, 8):
            inverse_ref[k, r : r + 8] = inverse_rows(cols_ref[k, r : r + 8])

    own_east, own_north = ice(me, values_ref)
    invert(count - 1)
    returned_ref[me, 0] = own_east
    returned_ref[me, 1] = own_north

    rim = rim_moves(
        sizes, body_ref, edge, east_ref, west_ref, south_ref, north_ref, send_rim, recv_rim
    )
    for copy in rim:
        copy.start()

    def step(k, carry):
        out_copy(k).wait_recv()
        pz, pm = behind(k)
        east, north = ice(pz * nm + pm, arrived)
        drag[k, 0] = east
        drag[k, 1] = north
        invert(k)

        @pl.when(k > 0)
        def _():
            back_copy(k - 1).start()

        return carry

    lax.fori_loop(0, count - 1, step, 0)
    back_copy(count - 2).start()

    for copy in rim:
        copy.wait()
    tall, wide = rows + 2 * ROW_RIM, width + LANES
    half = tall // 2
    wide_tiles = wide // LANES
    known = known_rows(sizes, rows, tall)
    has_south, has_north = m < nm - 1, m > 0
    extra = extra_columns(west_ref, rows)
    for k, east_at, west_at in rim_lanes(body_ref.shape[0]):
        for t in range(tiles):
            part = slice(t * LANES, (t + 1) * LANES)
            field[t, :rows] = body_ref[k, :, part]
            field[t, rows : rows + ROW_RIM] = jnp.where(has_south, south_ref[k, :, part], 0.0)
            field[t, rows + ROW_RIM :] = jnp.where(has_north, north_ref[k, :, part], 0.0)
        field[tiles] = rim_tile(k, east_at, west_at, east_ref, west_ref, extra, rows, known)
        for t in range(wide_tiles):
            part = slice(t * LANES, (t + 1) * LANES)
            halves_ref[k, 0, :, part] = field[t, pl.ds(0, half, stride=2), :]
            halves_ref[k, 1, :, part] = field[t, pl.ds(1, half, stride=2), :]

    def collect(i, carry):
        group = group_of(i)

        def arrive(k, inner):
            back_copy(k).wait_recv()
            return inner

        lax.fori_loop(i * per, jnp.minimum(i * per + per, count - 1), arrive, 0)
        added = put_group(
            group * per, per, returned_ref, inverse_ref, lanes_ref, group, rows * tiles
        )

        @pl.when(i == 0)
        def _():
            total[...] = added

        @pl.when(i > 0)
        def _():
            total[...] += added

        return carry

    lax.fori_loop(0, groups, collect, 0)
    for c in range(2):
        for j in range(tiles):
            stress_ref[c, :, j * LANES : (j + 1) * LANES] = total[
                j * rows : (j + 1) * rows, c * LANES : (c + 1) * LANES
            ]
    pack_edges([stress_ref.at[0], stress_ref.at[1]], stress_edge)
    late = around(
        sizes, stress_ref, stress_edge, late_east, late_west, late_south, late_north,
        send_late, recv_late,
    )
    for copy in late:
        copy.start()

    def finish(k, carry):
        out_copy(k).wait_send()
        back_copy(k).wait_send()
        return carry

    lax.fori_loop(0, count - 1, finish, 0)
    for copy in late:
        copy.wait()


def pack_edges(refs, edge_ref):
    rows, width = refs[0].shape
    per = LANES // COL_RIM
    slot = lax.broadcasted_iota(jnp.int32, (rows, LANES), 1) // COL_RIM
    for start in range(0, len(refs), per):
        tile = start // per
        first = jnp.zeros((rows, LANES), jnp.float32)
        last = first
        for k, ref in enumerate(refs[start : start + per]):
            head = ref[:, :LANES]
            tail = ref[:, width - LANES :]
            if k:
                head = pltpu.roll(head, k * COL_RIM, 1)
            if (k + 1) * COL_RIM != LANES:
                tail = pltpu.roll(tail, (k + 1) * COL_RIM, 1)
            first = jnp.where(slot == k, head, first)
            last = jnp.where(slot == k, tail, last)
        edge_ref[0, :, tile * LANES : (tile + 1) * LANES] = first
        edge_ref[1, :, tile * LANES : (tile + 1) * LANES] = last


def prepare_kernel(sea_ref, forcing_ref, weights_ref, excess_ref, mask_ref, out_ref, edge_ref):
    total = weights_ref[0]
    for k in range(1, 8):
        total = total + weights_ref[k]
    ocean = mask_ref[...] > 0
    inverse = jnp.where(ocean, 1.0 / ((1.0 + excess_ref[...]) * total), 0.0)
    for k in range(8):
        out_ref[k] = weights_ref[k] * inverse
    out_ref[8] = inverse
    out_ref[9] = jnp.where(ocean, sea_ref[...], 0.0)
    out_ref[10] = forcing_ref[...]
    pack_rims(out_ref, edge_ref)


def sweep_kernel(
    sizes,
    halves_ref, stress_ref, late_east, late_west, late_south, late_north, velocity_ref,
    out_ref, velocity_hbm,
    wide_ref, tile_ref, even_ref, odd_ref, write,
):
    _, rows, width = stress_ref.shape
    tall, wide = rows + 2 * ROW_RIM, width + LANES
    half = tall // 2
    tiles = wide // LANES
    write_velocity = pltpu.make_async_copy(velocity_ref, velocity_hbm, write)
    write_velocity.start()
    m = lax.axis_index("mer")
    has_south, has_north = m < sizes[1] - 1, m > 0
    known = known_rows(sizes, rows, tall)
    for c in range(2):
        wide_ref[c, :rows, :width] = stress_ref[c]
        wide_ref[c, rows : rows + ROW_RIM, :width] = jnp.where(has_south, late_south[c], 0.0)
        wide_ref[c, rows + ROW_RIM :, :width] = jnp.where(has_north, late_north[c], 0.0)
        wide_ref[c, :, width:] = side_tile(c, late_east, late_west, known)
    east_stress = wide_ref[0]
    north_stress = wide_ref[1]
    change = (
        pltpu.roll(north_stress, wide - 1, 1)
        - pltpu.roll(north_stress, 1, 1)
        - pltpu.roll(east_stress, tall - 1, 0)
        + pltpu.roll(east_stress, 1, 0)
    )
    for t in range(tiles):
        tile_ref[t] = change[:, t * LANES : (t + 1) * LANES]

    def take(k, which):
        return halves_ref[k, which]

    for which in range(2):
        rows_of = pl.ds(which, half, stride=2)
        for t in range(tiles):
            part = slice(t * LANES, (t + 1) * LANES)
            wide_ref[which, :half, part] = (
                halves_ref[10, which, :, part] + tile_ref[t, rows_of, :]
            ) * halves_ref[8, which, :, part]

    column_odd = lax.broadcasted_iota(jnp.int32, (half, wide), 1) % 2
    even_ref[...] = take(9, 0)
    odd_ref[...] = take(9, 1)

    def phase(own_ref, other_ref, odd, colours):
        base = wide_ref[odd, :half]
        other = other_ref[...]
        if odd:
            above, below = other, pltpu.roll(other, half - 1, 0)
        else:
            above, below = pltpu.roll(other, 1, 0), other
        base = base + take(2, odd) * below + take(3, odd) * above
        base = base + take(4, odd) * pltpu.roll(below, wide - 1, 1)
        base = base + take(5, odd) * pltpu.roll(below, 1, 1)
        base = base + take(6, odd) * pltpu.roll(above, wide - 1, 1)
        base = base + take(7, odd) * pltpu.roll(above, 1, 1)
        own = own_ref[...]
        for parity in colours:
            new = base + take(0, odd) * pltpu.roll(own, wide - 1, 1)
            new = new + take(1, odd) * pltpu.roll(own, 1, 1)
            own = jnp.where(column_odd == parity, new, own)
        own_ref[...] = own

    runs = [(0, [0, 1])]
    for _ in range(SWEEPS):
        runs += [(1, [0, 1, 0]), (0, [1, 0, 1])]
    runs[-1] = (0, [1, 0])
    for odd, colours in runs:
        if odd:
            phase(odd_ref, even_ref, 1, colours)
        else:
            phase(even_ref, odd_ref, 0, colours)
    for t in range(tiles - 1):
        part = slice(t * LANES, (t + 1) * LANES)
        tile_ref[t, pl.ds(0, rows // 2, stride=2), :] = even_ref[: rows // 2, part]
        tile_ref[t, pl.ds(1, rows // 2, stride=2), :] = odd_ref[: rows // 2, part]
        out_ref[:, part] = tile_ref[t, :rows, :]
    write_velocity.wait()


def local(
    sea_level,
    forcing,
    link_weights,
    excess,
    ocean_mask,
    current,
    intersection_block,
    intersection_cols,
    ice_mass,
    coriolis,
    ice_start,
    wind_stress,
):
    rows, width = sea_level.shape
    _, devices, pairs, block = intersection_cols.shape
    slots = devices * pairs
    tiles = width // LANES
    f32 = jnp.float32
    ice_shape = (devices, pairs, block)
    slot_bytes = slots * block * 4
    sizes = (lax.axis_size("zon"), lax.axis_size("mer"))
    arrays = 11
    tall, wide = rows + 2 * ROW_RIM, width + LANES
    dma = pltpu.SemaphoreType.DMA
    shape = jax.ShapeDtypeStruct
    stay = functools.partial(pltpu.with_memory_space_constraint, memory_space=pltpu.HBM)
    velocity, halves, *late = pl.pallas_call(
        functools.partial(travel_kernel, sizes),
        out_shape=(
            shape((2,) + ice_shape, f32),
            shape((arrays, 2, tall // 2, wide), f32),
            shape((2, rows, width), f32),
            shape((tall, LANES), f32),
            shape((tall, LANES), f32),
            shape((2, ROW_RIM, width), f32),
            shape((2, ROW_RIM, width), f32),
        ),
        in_specs=[HBM] * 12,
        out_specs=(VM,) * 7,
        scratch_shapes=[
            pltpu.VMEM((2, rows, width), f32),
            pltpu.VMEM((devices, pairs), jnp.int32),
            pltpu.VMEM((LANES, LANES), jnp.int32),
            pltpu.VMEM(ice_shape, jnp.int32),
            pltpu.VMEM(ice_shape, f32),
            pltpu.VMEM(ice_shape, f32),
            pltpu.VMEM((2,) + ice_shape, f32),
            pltpu.VMEM((2,) + ice_shape, f32),
            pltpu.VMEM((rows, width), f32),
            pltpu.VMEM((rows, width), f32),
            pltpu.VMEM((8, rows, width), f32),
            pltpu.VMEM((rows, width), f32),
            pltpu.VMEM((rows, width), jnp.int32),
            pltpu.VMEM((3, rows * tiles, 2 * LANES), jnp.bfloat16),
            pltpu.VMEM((slots // LANES, 8, LANES), jnp.int32),
            pltpu.VMEM((devices, 2, pairs, block), f32),
            pltpu.VMEM((devices, 2, pairs, block), f32),
            pltpu.VMEM((devices, 2, pairs, block), f32),
            pltpu.VMEM((devices, 2, pairs, block), f32),
            pltpu.VMEM(ice_shape, jnp.int32),
            pltpu.VMEM((rows * tiles, 2 * LANES), f32),
            pltpu.VMEM((arrays, rows, width), f32),
            pltpu.VMEM((2, rows + ROW_RIM, LANES), f32),
            pltpu.VMEM((tall, LANES), f32),
            pltpu.VMEM((rows + 5 * ROW_RIM, LANES), f32),
            pltpu.VMEM((arrays, ROW_RIM, width), f32),
            pltpu.VMEM((arrays, ROW_RIM, width), f32),
            pltpu.VMEM((wide // LANES, tall, LANES), f32),
            pltpu.VMEM((2, rows, LANES), f32),
            dma((12,)),
            dma((devices,)),
            dma((devices,)),
            dma((devices,)),
            dma((devices,)),
            dma((10,)),
            dma((10,)),
            dma((8,)),
            dma((8,)),
        ],
        compiler_params=pltpu.CompilerParams(
            vmem_limit_bytes=TRAVEL_VMEM, collective_id=0, has_side_effects=True
        ),
        cost_estimate=cost(slots * block * 4096, 16 * slot_bytes),
        name="travel",
    )(
        stay(current),
        stay(intersection_block),
        stay(intersection_cols),
        stay(ice_mass),
        stay(coriolis),
        stay(ice_start),
        stay(wind_stress),
        stay(sea_level),
        stay(forcing),
        stay(link_weights),
        stay(excess),
        stay(ocean_mask),
    )
    surface, velocity = pl.pallas_call(
        functools.partial(sweep_kernel, sizes),
        out_shape=(shape((rows, width), f32), shape((2,) + ice_shape, f32)),
        in_specs=[VM] * 7,
        out_specs=(VM, HBM),
        scratch_shapes=[
            pltpu.VMEM((2, tall, wide), f32),
            pltpu.VMEM((wide // LANES, tall, LANES), f32),
            pltpu.VMEM((tall // 2, wide), f32),
            pltpu.VMEM((tall // 2, wide), f32),
            dma,
        ],
        compiler_params=pltpu.CompilerParams(vmem_limit_bytes=SWEEP_VMEM),
        cost_estimate=cost(rows * width * 200, rows * width * 64),
        name="sweep",
    )(halves, *late, velocity)
    return (surface, velocity.reshape((2, 1) + ice_shape))


def solution(mesh):
    return jax.shard_map(
        local,
        mesh=mesh,
        in_specs=(
            P("mer", "zon"),
            P("mer", "zon"),
            P(None, "mer", "zon"),
            P("mer", "zon"),
            P("mer", "zon"),
            P(None, "mer", "zon"),
            P(("zon", "mer"), None, None),
            P(("zon", "mer"), None, None, None),
            P(("zon", "mer"), None, None, None),
            P(("zon", "mer"), None, None, None),
            P(None, ("zon", "mer"), None, None, None),
            P(None, ("zon", "mer"), None, None, None),
        ),
        out_specs=(P("mer", "zon"), P(None, ("zon", "mer"), None, None, None)),
        check_vma=False,
    )
```

```python
import functools

import jax
import jax.numpy as jnp
from jax import lax
from jax.experimental import pallas as pl
from jax.experimental.pallas import tpu as pltpu
from jax.sharding import PartitionSpec as P

SWEEPS = 2
ICE_SWEEPS = 3
ROW_RIM = 8
COL_RIM = 16
LANES = 128
EAST_COLS = 11
WEST_COLS = 12
EXTRA_COLS = 8
FIELD = 9

drag_coeff = 1.0
link_coeff = 0.5
VM = pl.BlockSpec(memory_space=pltpu.VMEM)
HBM = pl.BlockSpec(memory_space=pltpu.HBM)
TRAVEL_VMEM = 40 * 1024 * 1024
SWEEP_VMEM = 16 * 1024 * 1024


def cost(flops, nbytes):
    return pl.CostEstimate(flops=flops, bytes_accessed=nbytes, transcendentals=0)


def lane_take(values, index):
    return jnp.take_along_axis(values, index, axis=1, mode="promise_in_bounds")


def split3(values):
    high = values.astype(jnp.bfloat16)
    rest = values - high.astype(jnp.float32)
    middle = rest.astype(jnp.bfloat16)
    low = (rest - middle.astype(jnp.float32)).astype(jnp.bfloat16)
    return high, middle, low


def nn_dot(a, b):
    return lax.dot_general(a, b, (((1,), (0,)), ((), ())), preferred_element_type=jnp.float32)


def block_rows(blocks, tiles, rows):
    safe = jnp.maximum(blocks, 0)
    return jnp.where(blocks >= 0, (safe % tiles) * rows + safe // tiles, -1)


def inverse_rows(cols):
    lane = lax.broadcasted_iota(jnp.int32, (8, LANES), 1)
    sub = lax.broadcasted_iota(jnp.int32, (8, LANES), 0)
    order = (lane + 1).astype(jnp.float32)
    index = (lane % 16) * 8 + sub
    group = lane // 16
    high = jnp.right_shift(cols, 4)
    low = jnp.bitwise_and(cols, 15)
    left = jnp.concatenate([jnp.where(high == h, 1.0, 0.0) for h in range(8)], axis=0)
    right = jnp.concatenate([jnp.where(low == b, order, 0.0) for b in range(16)], axis=0)
    product = lax.dot_general(
        left.astype(jnp.bfloat16),
        right.astype(jnp.bfloat16),
        (((1,), (1,)), ((), ())),
        preferred_element_type=jnp.float32,
    )
    found = jnp.zeros((8, LANES), jnp.float32)
    for h in range(8):
        found = jnp.where(group == h, lane_take(product[h * 8 : (h + 1) * 8], index), found)
    return found.astype(jnp.int32) - 1


def ice_block(mass, coriolis, start, wind, current):
    pairs, width = mass.shape
    lane = lax.broadcasted_iota(jnp.int32, (pairs, width), 1)
    first, last = lane == 0, lane == width - 1

    def beside(values):
        before = jnp.where(first, 0.0, pltpu.roll(values, 1, 1))
        after = jnp.where(last, 0.0, pltpu.roll(values, width - 1, 1))
        return before + after

    diagonal = mass + drag_coeff + 2.0 * link_coeff
    turning = coriolis * mass
    inverse = 1.0 / (diagonal * diagonal + turning * turning)
    diagonal = diagonal * inverse
    turning = turning * inverse
    east, north = start
    base_east = mass * east + wind[0] + drag_coeff * current[0]
    base_north = mass * north + wind[1] + drag_coeff * current[1]
    for _ in range(ICE_SWEEPS):
        right_east = base_east + link_coeff * beside(east)
        right_north = base_north + link_coeff * beside(north)
        east = diagonal * right_east + turning * right_north
        north = diagonal * right_north - turning * right_east
    return east, north


def around(sizes, body_ref, edge_ref, east_ref, west_ref, south_ref, north_ref, send, recv):
    rows = body_ref.shape[1]
    top, end = pl.ds(0, ROW_RIM), pl.ds(rows - ROW_RIM, ROW_RIM)
    whole, after, before = pl.ds(0, rows), pl.ds(rows, ROW_RIM), pl.ds(rows + ROW_RIM, ROW_RIM)
    moves = [
        (edge_ref.at[0], east_ref.at[whole], -1, 0),
        (edge_ref.at[1], west_ref.at[whole], 1, 0),
        (body_ref.at[:, top], south_ref, 0, -1),
        (body_ref.at[:, end], north_ref, 0, 1),
        (edge_ref.at[0, top], east_ref.at[after], -1, -1),
        (edge_ref.at[0, end], east_ref.at[before], -1, 1),
        (edge_ref.at[1, top], west_ref.at[after], 1, -1),
        (edge_ref.at[1, end], west_ref.at[before], 1, 1),
    ]
    return neighbour_copies(sizes, moves, send, recv)


def neighbour_copies(sizes, moves, send, recv):
    nz, nm = sizes
    z, m = lax.axis_index("zon"), lax.axis_index("mer")
    return [
        pltpu.make_async_remote_copy(
            src_ref=source,
            dst_ref=target,
            send_sem=send.at[i],
            recv_sem=recv.at[i],
            device_id={"zon": lax.rem(z + dz + nz, nz), "mer": lax.rem(m + dm + nm, nm)},
            device_id_type=pl.DeviceIdType.MESH,
        )
        for i, (source, target, dz, dm) in enumerate(moves)
    ]


def pick_group(base, per, turned_ids, parts, cols_ref, values_ref, lanes_ref, group):
    pairs = cols_ref.shape[1]
    lane = lax.broadcasted_iota(jnp.int32, (LANES, LANES), 1)
    turned = jnp.concatenate(
        [
            lane_take(turned_ids, jnp.full((pairs, LANES), base + d, jnp.int32))
            for d in range(per)
        ],
        axis=0,
    )
    lanes_ref[group] = jnp.transpose(turned)[:8]
    pick = jnp.concatenate(
        [
            jnp.where(turned == lane + b * LANES, 1.0, 0.0).astype(jnp.bfloat16)
            for b in range(parts.shape[1] // LANES)
        ],
        axis=1,
    )
    picked = nn_dot(pick, parts[0]) + nn_dot(pick, parts[1]) + nn_dot(pick, parts[2])
    cols = cols_ref[pl.ds(base, per)].reshape(LANES, LANES)
    index = jnp.maximum(cols, 0)
    for c in range(2):
        taken = lane_take(picked[:, c * LANES : (c + 1) * LANES], index)
        taken = jnp.where(cols >= 0, taken, 0.0)
        for d in range(per):
            values_ref[base + d, c] = taken[d * pairs : (d + 1) * pairs]


def put_group(base, per, returned_ref, inverse_ref, lanes_ref, group, count):
    pairs = inverse_ref.shape[1]
    row = lax.broadcasted_iota(jnp.int32, (count, LANES), 0)
    ids = lanes_ref[group]
    put = jnp.where(
        jnp.broadcast_to(ids[:1], (count, LANES)) == row, 1.0, 0.0
    ).astype(jnp.bfloat16)
    inverse = inverse_ref[pl.ds(base, per)].reshape(LANES, LANES)
    index = jnp.maximum(inverse, 0)
    halves = []
    for c in range(2):
        values = jnp.concatenate([returned_ref[base + d, c] for d in range(per)], axis=0)
        halves.append(jnp.where(inverse >= 0, lane_take(values, index), 0.0))
    high, middle, low = split3(jnp.concatenate(halves, axis=1))
    return nn_dot(put, high) + nn_dot(put, middle) + nn_dot(put, low)


def side_tile(k, east_ref, west_ref, known):
    tall = east_ref.shape[0]
    per = LANES // COL_RIM
    slot = lax.broadcasted_iota(jnp.int32, (tall, LANES), 1) // COL_RIM
    at = (k // per) * LANES
    spot = k % per
    east = east_ref[:, at : at + LANES]
    west = west_ref[:, at : at + LANES]
    if spot:
        east = pltpu.roll(east, LANES - spot * COL_RIM, 1)
    if spot != per - 1:
        west = pltpu.roll(west, LANES - (spot + 1) * COL_RIM, 1)
    both = jnp.where(slot == 0, east, jnp.where(slot == per - 1, west, 0.0))
    return jnp.where(known, both, 0.0)


def known_rows(sizes, rows, tall):
    m = lax.axis_index("mer")
    row = lax.broadcasted_iota(jnp.int32, (tall, LANES), 0)
    lower = jnp.where(m == sizes[1] - 1, rows, rows + ROW_RIM)
    upper = jnp.where(m == 0, tall, rows + ROW_RIM)
    return (row < lower) | ((row >= rows + ROW_RIM) & (row >= upper))


def split_columns(tiles):
    rows = tiles[0].shape[0]
    lane = lax.broadcasted_iota(jnp.int32, (rows, LANES), 1)
    half = LANES // 2
    index = 2 * (lane % half) + lane // half
    low = lane < half
    here = [lane_take(tile, index) for tile in tiles]
    away = [pltpu.roll(tile, half, 1) for tile in here]
    even, odd = [], []
    for t in range(0, len(tiles), 2):
        u = min(t + 1, len(tiles) - 1)
        even.append(jnp.where(low, here[t], away[u]))
        odd.append(jnp.where(low, away[t], here[u]))
    return even, odd


def join_columns(even, odd, tile):
    rows = even.shape[0]
    lane = lax.broadcasted_iota(jnp.int32, (rows, LANES), 1)
    index = (tile % 2) * (LANES // 2) + lane // 2
    return jnp.where(lane % 2 == 0, lane_take(even, index), lane_take(odd, index))


def rim_lanes(arrays):
    order = [k for k in range(arrays) if k != FIELD] + [FIELD]
    return [(k, i * EAST_COLS, i * WEST_COLS) for i, k in enumerate(order)]


def pack_rims(body_ref, edge_ref):
    arrays, rows, width = body_ref.shape
    lane = lax.broadcasted_iota(jnp.int32, (rows, LANES), 1)
    first = jnp.zeros((rows, LANES), jnp.float32)
    last = first
    for k, east, west in rim_lanes(arrays):
        head = body_ref[k, :, :LANES]
        tail = body_ref[k, :, width - LANES :]
        if east:
            head = pltpu.roll(head, east, 1)
        first = jnp.where(lane >= east, head, first)
        if k == FIELD:
            last = jnp.where(lane >= west, tail, last)
        else:
            tail = pltpu.roll(tail, west + WEST_COLS, 1)
            last = jnp.where((lane >= west) & (lane < west + WEST_COLS), tail, last)
    edge_ref[0, :rows] = first
    edge_ref[1, :rows] = last
    near = lane[:ROW_RIM]
    extra = jnp.zeros((ROW_RIM, LANES), jnp.float32)
    for g in range(rows // ROW_RIM):
        piece = body_ref[FIELD, g * ROW_RIM : (g + 1) * ROW_RIM, width - LANES :]
        at = g * EXTRA_COLS
        shift = (at + COL_RIM) % LANES
        if shift:
            piece = pltpu.roll(piece, shift, 1)
        extra = jnp.where((near >= at) & (near < at + EXTRA_COLS), piece, extra)
    edge_ref[1, rows : rows + ROW_RIM] = extra
    edge_ref[0, rows : rows + ROW_RIM] = extra


def rim_moves(sizes, body_ref, edge_ref, east_ref, west_ref, south_ref, north_ref, send, recv):
    rows = body_ref.shape[1]
    end = rows - ROW_RIM

    def part(at, count=ROW_RIM):
        return pl.ds(at, count)

    return neighbour_copies(
        sizes,
        [
            (edge_ref.at[0, part(0, rows)], east_ref.at[part(0, rows)], -1, 0),
            (edge_ref.at[1], west_ref.at[part(0, rows + ROW_RIM)], 1, 0),
            (body_ref.at[:, part(0)], south_ref, 0, -1),
            (body_ref.at[:, part(end)], north_ref, 0, 1),
            (edge_ref.at[0, part(0)], east_ref.at[part(rows)], -1, -1),
            (edge_ref.at[0, part(end)], east_ref.at[part(rows + ROW_RIM)], -1, 1),
            (edge_ref.at[1, part(0)], west_ref.at[part(rows + ROW_RIM)], 1, -1),
            (edge_ref.at[1, part(end)], west_ref.at[part(rows + 2 * ROW_RIM)], 1, 1),
            (edge_ref.at[1, part(rows)], west_ref.at[part(rows + 3 * ROW_RIM)], 1, -1),
            (edge_ref.at[1, part(rows)], west_ref.at[part(rows + 4 * ROW_RIM)], 1, 1),
        ],
        send,
        recv,
    )


def extra_columns(west_ref, rows):
    pieces = []
    for g in range(rows // ROW_RIM):
        shift = (2 * LANES - COL_RIM - g * EXTRA_COLS) % LANES
        piece = west_ref[rows : rows + ROW_RIM]
        pieces.append(pltpu.roll(piece, shift, 1) if shift else piece)
    south = west_ref[rows + 3 * ROW_RIM : rows + 4 * ROW_RIM]
    north = west_ref[rows + 4 * ROW_RIM : rows + 5 * ROW_RIM]
    pieces.append(pltpu.roll(south, LANES - COL_RIM, 1))
    last = (2 * LANES - COL_RIM - (rows // ROW_RIM - 1) * EXTRA_COLS) % LANES
    pieces.append(pltpu.roll(north, last, 1) if last else north)
    return jnp.concatenate(pieces, axis=0)


def rim_tile(k, east_at, west_at, east_ref, west_ref, extra, rows, known):
    tall = rows + 2 * ROW_RIM
    lane = lax.broadcasted_iota(jnp.int32, (tall, LANES), 1)
    east = east_ref[...]
    west = jnp.concatenate(
        [west_ref[:rows], west_ref[rows + ROW_RIM : rows + 3 * ROW_RIM]], axis=0
    )
    if east_at:
        east = pltpu.roll(east, LANES - east_at, 1)
    if k == FIELD:
        kept, near = EAST_COLS + 1, LANES - (LANES - west_at)
        west = jnp.where(lane >= near, west, extra)
        first = LANES - COL_RIM
    else:
        kept, first = EAST_COLS, LANES - WEST_COLS
        west = pltpu.roll(west, LANES - west_at - WEST_COLS, 1)
    both = jnp.where(lane < kept, east, jnp.where(lane >= first, west, 0.0))
    return jnp.where(known, both, 0.0)


def travel_kernel(
    sizes,
    current_hbm, blocks_hbm, cols_hbm, mass_hbm, coriolis_hbm, start_hbm, wind_hbm,
    sea_hbm, forcing_hbm, weights_hbm, excess_hbm, mask_hbm,
    velocity_ref, halves_ref, stress_ref, late_east, late_west, late_south, late_north,
    current_ref, blocks_ref, square, cols_ref, mass_ref, coriolis_ref, start_ref, wind_ref,
    sea_ref, forcing_ref, weights_ref, excess_ref, mask_ref,
    parts, lanes_ref, values_ref, arrived, drag, returned_ref, inverse_ref, total,
    body_ref, edge, east_ref, west_ref, south_ref, north_ref, field, stress_edge,
    loads, send_out, recv_out, send_back, recv_back, send_rim, recv_rim, send_late, recv_late,
):
    nz, nm = sizes
    count = nz * nm
    z, m = lax.axis_index("zon"), lax.axis_index("mer")
    me = z * nm + m
    _, rows, width = current_ref.shape
    tiles = width // LANES
    devices, pairs, _ = cols_ref.shape
    per = LANES // pairs
    span = per // nm
    groups = count // per
    mine = lax.div(z, span)

    def group_of(i):
        return lax.rem(mine + groups // 2 + lax.div(i + 1, 2) * (1 - 2 * lax.rem(i, 2)), groups)

    def group_from(i):
        return lax.rem(
            mine + groups + groups // 2 - lax.div(i + 1, 2) * (1 - 2 * lax.rem(i, 2)), groups
        )

    def member(group, k):
        inner = lax.rem(k, per)
        a = lax.rem(lax.rem(z, span) + span - 1 - lax.div(inner, nm), span)
        return group * span + a, lax.rem(m + nm - 1 - lax.rem(inner, nm), nm)

    def member_from(group, k):
        inner = lax.rem(k, per)
        a = lax.rem(lax.rem(z, span) + 1 + lax.div(inner, nm), span)
        return group * span + a, lax.rem(m + 1 + lax.rem(inner, nm), nm)

    def ahead(k):
        return member(group_of(lax.div(k, per)), k)

    def behind(k):
        return member_from(group_from(lax.div(k, per)), k)

    def out_copy(k):
        pz, pm = ahead(k)
        return pltpu.make_async_remote_copy(
            src_ref=values_ref.at[pz * nm + pm],
            dst_ref=arrived.at[me],
            send_sem=send_out.at[k],
            recv_sem=recv_out.at[k],
            device_id={"zon": pz, "mer": pm},
            device_id_type=pl.DeviceIdType.MESH,
        )

    def back_copy(k):
        pz, pm = behind(k)
        return pltpu.make_async_remote_copy(
            src_ref=drag.at[k],
            dst_ref=returned_ref.at[me],
            send_sem=send_back.at[k],
            recv_sem=recv_back.at[k],
            device_id={"zon": pz, "mer": pm},
            device_id_type=pl.DeviceIdType.MESH,
        )

    barrier = pltpu.get_barrier_semaphore()

    def greet(k, carry):
        pz, pm = ahead(k)
        pl.semaphore_signal(
            barrier,
            inc=1,
            device_id={"zon": pz, "mer": pm},
            device_id_type=pl.DeviceIdType.MESH,
        )
        return carry

    copies = [
        pltpu.make_async_copy(source, target, loads.at[i])
        for i, (source, target) in enumerate(
            [
                (current_hbm, current_ref),
                (blocks_hbm.at[0], blocks_ref),
                (cols_hbm.at[0], cols_ref),
                (mass_hbm.at[0], mass_ref),
                (coriolis_hbm.at[0], coriolis_ref),
                (start_hbm.at[:, 0], start_ref),
                (wind_hbm.at[:, 0], wind_ref),
                (weights_hbm, weights_ref),
                (sea_hbm, sea_ref),
                (forcing_hbm, forcing_ref),
                (excess_hbm, excess_ref),
                (mask_hbm, mask_ref),
            ]
        )
    ]
    for copy in copies:
        copy.start()
    lax.fori_loop(0, count - 1, greet, 0)

    copies[0].wait()
    for j in range(tiles):
        for c in range(2):
            for k, part in enumerate(split3(current_ref[c, :, j * LANES : (j + 1) * LANES])):
                parts[k, j * rows : (j + 1) * rows, c * LANES : (c + 1) * LANES] = part
    copies[1].wait()
    square[:devices, :pairs] = block_rows(blocks_ref[...], tiles, rows)
    turned_ids = jnp.transpose(square[...])[:pairs]
    copies[2].wait()

    def pick(i, carry):
        group = group_of(i)
        pick_group(group * per, per, turned_ids, parts, cols_ref, values_ref, lanes_ref, group)
        return carry

    def launch(k, carry):
        out_copy(k).start()
        return carry

    first = min(2, groups)
    lax.fori_loop(0, first, pick, 0)
    pl.semaphore_wait(barrier, count - 1)

    def pick_and_launch(i, carry):
        lax.fori_loop((i - first) * per, (i - first + 1) * per, launch, 0)
        return pick(i, carry)

    lax.fori_loop(first, groups, pick_and_launch, 0)
    lax.fori_loop((groups - first) * per, count - 1, launch, 0)

    for copy in copies[3:]:
        copy.wait()
    prepare_kernel(sea_ref, forcing_ref, weights_ref, excess_ref, mask_ref, body_ref, edge)

    def ice(at, from_ref):
        current = (from_ref[at, 0], from_ref[at, 1])
        east, north = ice_block(
            mass_ref[at],
            coriolis_ref[at],
            (start_ref[0, at], start_ref[1, at]),
            (wind_ref[0, at], wind_ref[1, at]),
            current,
        )
        velocity_ref[0, at] = east
        velocity_ref[1, at] = north
        return drag_coeff * (east - current[0]), drag_coeff * (north - current[1])

    def invert(k):
        for r in range(0, pairs, 8):
            inverse_ref[k, r : r + 8] = inverse_rows(cols_ref[k, r : r + 8])

    own_east, own_north = ice(me, values_ref)
    invert(count - 1)
    returned_ref[me, 0] = own_east
    returned_ref[me, 1] = own_north

    rim = rim_moves(
        sizes, body_ref, edge, east_ref, west_ref, south_ref, north_ref, send_rim, recv_rim
    )
    for copy in rim:
        copy.start()

    def step(k, carry):
        out_copy(k).wait_recv()
        pz, pm = behind(k)
        east, north = ice(pz * nm + pm, arrived)
        drag[k, 0] = east
        drag[k, 1] = north
        invert(k)

        @pl.when(k > 0)
        def _():
            back_copy(k - 1).start()

        return carry

    lax.fori_loop(0, count - 1, step, 0)
    back_copy(count - 2).start()

    for copy in rim:
        copy.wait()
    tall, wide = rows + 2 * ROW_RIM, width + LANES
    half = tall // 2
    wide_tiles = wide // LANES
    known = known_rows(sizes, rows, tall)
    has_south, has_north = m < nm - 1, m > 0
    extra = extra_columns(west_ref, rows)
    for k, east_at, west_at in rim_lanes(body_ref.shape[0]):
        for t in range(tiles):
            part = slice(t * LANES, (t + 1) * LANES)
            field[t, :rows] = body_ref[k, :, part]
            field[t, rows : rows + ROW_RIM] = jnp.where(has_south, south_ref[k, :, part], 0.0)
            field[t, rows + ROW_RIM :] = jnp.where(has_north, north_ref[k, :, part], 0.0)
        field[tiles] = rim_tile(k, east_at, west_at, east_ref, west_ref, extra, rows, known)
        for which in range(2):
            rows_of = pl.ds(which, half, stride=2)
            split = split_columns([field[t, rows_of, :] for t in range(wide_tiles)])
            for odd, found in enumerate(split):
                whole = jnp.concatenate(found, axis=1)
                if k in (4, 6) and odd:
                    whole = pltpu.roll(whole, 1, 1)
                if k in (5, 7) and not odd:
                    whole = pltpu.roll(whole, whole.shape[1] - 1, 1)
                halves_ref[k, which, odd] = whole

    def collect(i, carry):
        group = group_of(i)

        def arrive(k, inner):
            back_copy(k).wait_recv()
            return inner

        lax.fori_loop(i * per, jnp.minimum(i * per + per, count - 1), arrive, 0)
        added = put_group(
            group * per, per, returned_ref, inverse_ref, lanes_ref, group, rows * tiles
        )

        @pl.when(i == 0)
        def _():
            total[...] = added

        @pl.when(i > 0)
        def _():
            total[...] += added

        return carry

    lax.fori_loop(0, groups, collect, 0)
    for c in range(2):
        for j in range(tiles):
            stress_ref[c, :, j * LANES : (j + 1) * LANES] = total[
                j * rows : (j + 1) * rows, c * LANES : (c + 1) * LANES
            ]
    pack_edges([stress_ref.at[0], stress_ref.at[1]], stress_edge)
    late = around(
        sizes, stress_ref, stress_edge, late_east, late_west, late_south, late_north,
        send_late, recv_late,
    )
    for copy in late:
        copy.start()

    def finish(k, carry):
        out_copy(k).wait_send()
        back_copy(k).wait_send()
        return carry

    lax.fori_loop(0, count - 1, finish, 0)
    for copy in late:
        copy.wait()


def pack_edges(refs, edge_ref):
    rows, width = refs[0].shape
    per = LANES // COL_RIM
    slot = lax.broadcasted_iota(jnp.int32, (rows, LANES), 1) // COL_RIM
    for start in range(0, len(refs), per):
        tile = start // per
        first = jnp.zeros((rows, LANES), jnp.float32)
        last = first
        for k, ref in enumerate(refs[start : start + per]):
            head = ref[:, :LANES]
            tail = ref[:, width - LANES :]
            if k:
                head = pltpu.roll(head, k * COL_RIM, 1)
            if (k + 1) * COL_RIM != LANES:
                tail = pltpu.roll(tail, (k + 1) * COL_RIM, 1)
            first = jnp.where(slot == k, head, first)
            last = jnp.where(slot == k, tail, last)
        edge_ref[0, :, tile * LANES : (tile + 1) * LANES] = first
        edge_ref[1, :, tile * LANES : (tile + 1) * LANES] = last


def prepare_kernel(sea_ref, forcing_ref, weights_ref, excess_ref, mask_ref, out_ref, edge_ref):
    total = weights_ref[0]
    for k in range(1, 8):
        total = total + weights_ref[k]
    ocean = mask_ref[...] > 0
    inverse = jnp.where(ocean, 1.0 / ((1.0 + excess_ref[...]) * total), 0.0)
    for k in range(8):
        out_ref[k] = weights_ref[k] * inverse
    out_ref[8] = inverse
    out_ref[9] = jnp.where(ocean, sea_ref[...], 0.0)
    out_ref[10] = forcing_ref[...]
    pack_rims(out_ref, edge_ref)


def sweep_kernel(
    sizes,
    halves_ref, stress_ref, late_east, late_west, late_south, late_north, velocity_ref,
    out_ref, velocity_hbm,
    wide_ref, tile_ref, source_ref, field_ref, write,
):
    _, rows, width = stress_ref.shape
    tall, wide = rows + 2 * ROW_RIM, width + LANES
    half = tall // 2
    tiles = wide // LANES
    write_velocity = pltpu.make_async_copy(velocity_ref, velocity_hbm, write)
    write_velocity.start()
    m = lax.axis_index("mer")
    has_south, has_north = m < sizes[1] - 1, m > 0
    known = known_rows(sizes, rows, tall)
    for c in range(2):
        wide_ref[c, :rows, :width] = stress_ref[c]
        wide_ref[c, rows : rows + ROW_RIM, :width] = jnp.where(has_south, late_south[c], 0.0)
        wide_ref[c, rows + ROW_RIM :, :width] = jnp.where(has_north, late_north[c], 0.0)
        wide_ref[c, :, width:] = side_tile(c, late_east, late_west, known)
    east_stress = wide_ref[0]
    north_stress = wide_ref[1]
    change = (
        pltpu.roll(north_stress, wide - 1, 1)
        - pltpu.roll(north_stress, 1, 1)
        - pltpu.roll(east_stress, tall - 1, 0)
        + pltpu.roll(east_stress, 1, 0)
    )
    for t in range(tiles):
        tile_ref[t] = change[:, t * LANES : (t + 1) * LANES]

    thin = field_ref.shape[3]
    for which in range(2):
        rows_of = pl.ds(which, half, stride=2)
        split = split_columns([tile_ref[t, rows_of, :] for t in range(tiles)])
        for odd, found in enumerate(split):
            source_ref[which, odd] = (
                halves_ref[10, which, odd] + jnp.concatenate(found, axis=1)
            ) * halves_ref[8, which, odd]
            field_ref[which, odd] = halves_ref[FIELD, which, odd]

    def phase(which, colours):
        other = [field_ref[1 - which, odd] for odd in range(2)]
        if which:
            above = other
            below = [pltpu.roll(value, half - 1, 0) for value in other]
        else:
            above = [pltpu.roll(value, 1, 0) for value in other]
            below = other
        weight = [[halves_ref[k, which, odd] for k in range(8)] for odd in range(2)]
        w = weight[0]
        base_even = source_ref[which, 0] + w[2] * below[0] + w[3] * above[0]
        base_even = base_even + w[4] * below[1] + w[6] * above[1]
        base_even = base_even + pltpu.roll(w[5] * below[1] + w[7] * above[1], 1, 1)
        w = weight[1]
        base_odd = source_ref[which, 1] + w[2] * below[1] + w[3] * above[1]
        base_odd = base_odd + w[5] * below[0] + w[7] * above[0]
        base_odd = base_odd + pltpu.roll(w[4] * below[0] + w[6] * above[0], thin - 1, 1)
        even, odd = field_ref[which, 0], field_ref[which, 1]
        for parity in colours:
            if parity:
                odd = base_odd + weight[1][0] * pltpu.roll(even, thin - 1, 1)
                odd = odd + weight[1][1] * even
            else:
                even = base_even + weight[0][0] * odd
                even = even + weight[0][1] * pltpu.roll(odd, 1, 1)
        field_ref[which, 0] = even
        field_ref[which, 1] = odd

    runs = [(0, [0, 1])]
    for _ in range(SWEEPS):
        runs += [(1, [0, 1, 0]), (0, [1, 0, 1])]
    runs[-1] = (0, [1, 0])
    for which, colours in runs:
        phase(which, colours)
    for t in range(tiles - 1):
        at = slice(t // 2 * LANES, t // 2 * LANES + LANES)
        for which in range(2):
            tile_ref[t, pl.ds(which, rows // 2, stride=2), :] = join_columns(
                field_ref[which, 0, : rows // 2, at], field_ref[which, 1, : rows // 2, at], t
            )
        out_ref[:, t * LANES : (t + 1) * LANES] = tile_ref[t, :rows, :]
    write_velocity.wait()


def local(
    sea_level,
    forcing,
    link_weights,
    excess,
    ocean_mask,
    current,
    intersection_block,
    intersection_cols,
    ice_mass,
    coriolis,
    ice_start,
    wind_stress,
):
    rows, width = sea_level.shape
    _, devices, pairs, block = intersection_cols.shape
    slots = devices * pairs
    tiles = width // LANES
    f32 = jnp.float32
    ice_shape = (devices, pairs, block)
    slot_bytes = slots * block * 4
    sizes = (lax.axis_size("zon"), lax.axis_size("mer"))
    arrays = 11
    tall, wide = rows + 2 * ROW_RIM, width + LANES
    thin = -(-wide // (2 * LANES)) * LANES
    dma = pltpu.SemaphoreType.DMA
    shape = jax.ShapeDtypeStruct
    stay = functools.partial(pltpu.with_memory_space_constraint, memory_space=pltpu.HBM)
    velocity, halves, *late = pl.pallas_call(
        functools.partial(travel_kernel, sizes),
        out_shape=(
            shape((2,) + ice_shape, f32),
            shape((arrays, 2, 2, tall // 2, thin), f32),
            shape((2, rows, width), f32),
            shape((tall, LANES), f32),
            shape((tall, LANES), f32),
            shape((2, ROW_RIM, width), f32),
            shape((2, ROW_RIM, width), f32),
        ),
        in_specs=[HBM] * 12,
        out_specs=(VM,) * 7,
        scratch_shapes=[
            pltpu.VMEM((2, rows, width), f32),
            pltpu.VMEM((devices, pairs), jnp.int32),
            pltpu.VMEM((LANES, LANES), jnp.int32),
            pltpu.VMEM(ice_shape, jnp.int32),
            pltpu.VMEM(ice_shape, f32),
            pltpu.VMEM(ice_shape, f32),
            pltpu.VMEM((2,) + ice_shape, f32),
            pltpu.VMEM((2,) + ice_shape, f32),
            pltpu.VMEM((rows, width), f32),
            pltpu.VMEM((rows, width), f32),
            pltpu.VMEM((8, rows, width), f32),
            pltpu.VMEM((rows, width), f32),
            pltpu.VMEM((rows, width), jnp.int32),
            pltpu.VMEM((3, rows * tiles, 2 * LANES), jnp.bfloat16),
            pltpu.VMEM((slots // LANES, 8, LANES), jnp.int32),
            pltpu.VMEM((devices, 2, pairs, block), f32),
            pltpu.VMEM((devices, 2, pairs, block), f32),
            pltpu.VMEM((devices, 2, pairs, block), f32),
            pltpu.VMEM((devices, 2, pairs, block), f32),
            pltpu.VMEM(ice_shape, jnp.int32),
            pltpu.VMEM((rows * tiles, 2 * LANES), f32),
            pltpu.VMEM((arrays, rows, width), f32),
            pltpu.VMEM((2, rows + ROW_RIM, LANES), f32),
            pltpu.VMEM((tall, LANES), f32),
            pltpu.VMEM((rows + 5 * ROW_RIM, LANES), f32),
            pltpu.VMEM((arrays, ROW_RIM, width), f32),
            pltpu.VMEM((arrays, ROW_RIM, width), f32),
            pltpu.VMEM((wide // LANES, tall, LANES), f32),
            pltpu.VMEM((2, rows, LANES), f32),
            dma((12,)),
            dma((devices,)),
            dma((devices,)),
            dma((devices,)),
            dma((devices,)),
            dma((10,)),
            dma((10,)),
            dma((8,)),
            dma((8,)),
        ],
        compiler_params=pltpu.CompilerParams(
            vmem_limit_bytes=TRAVEL_VMEM, collective_id=0, has_side_effects=True
        ),
        cost_estimate=cost(slots * block * 4096, 16 * slot_bytes),
        name="travel",
    )(
        stay(current),
        stay(intersection_block),
        stay(intersection_cols),
        stay(ice_mass),
        stay(coriolis),
        stay(ice_start),
        stay(wind_stress),
        stay(sea_level),
        stay(forcing),
        stay(link_weights),
        stay(excess),
        stay(ocean_mask),
    )
    surface, velocity = pl.pallas_call(
        functools.partial(sweep_kernel, sizes),
        out_shape=(shape((rows, width), f32), shape((2,) + ice_shape, f32)),
        in_specs=[VM] * 7,
        out_specs=(VM, HBM),
        scratch_shapes=[
            pltpu.VMEM((2, tall, wide), f32),
            pltpu.VMEM((wide // LANES, tall, LANES), f32),
            pltpu.VMEM((2, 2, tall // 2, thin), f32),
            pltpu.VMEM((2, 2, tall // 2, thin), f32),
            dma,
        ],
        compiler_params=pltpu.CompilerParams(vmem_limit_bytes=SWEEP_VMEM),
        cost_estimate=cost(rows * width * 200, rows * width * 64),
        name="sweep",
    )(halves, *late, velocity)
    return (surface, velocity.reshape((2, 1) + ice_shape))


def solution(mesh):
    return jax.shard_map(
        local,
        mesh=mesh,
        in_specs=(
            P("mer", "zon"),
            P("mer", "zon"),
            P(None, "mer", "zon"),
            P("mer", "zon"),
            P("mer", "zon"),
            P(None, "mer", "zon"),
            P(("zon", "mer"), None, None),
            P(("zon", "mer"), None, None, None),
            P(("zon", "mer"), None, None, None),
            P(("zon", "mer"), None, None, None),
            P(None, ("zon", "mer"), None, None, None),
            P(None, ("zon", "mer"), None, None, None),
        ),
        out_specs=(P("mer", "zon"), P(None, ("zon", "mer"), None, None, None)),
        check_vma=False,
    )
```

```python
import functools

import jax
import jax.numpy as jnp
from jax import lax
from jax.experimental import pallas as pl
from jax.experimental.pallas import tpu as pltpu
from jax.sharding import PartitionSpec as P

SWEEPS = 2
ICE_SWEEPS = 3
ROW_RIM = 8
COL_RIM = 16
LANES = 128
EAST_COLS = 11
WEST_COLS = 12
EXTRA_COLS = 8
FIELD = 9

drag_coeff = 1.0
link_coeff = 0.5
VM = pl.BlockSpec(memory_space=pltpu.VMEM)
HBM = pl.BlockSpec(memory_space=pltpu.HBM)
TRAVEL_VMEM = 40 * 1024 * 1024
SWEEP_VMEM = 16 * 1024 * 1024


def cost(flops, nbytes):
    return pl.CostEstimate(flops=flops, bytes_accessed=nbytes, transcendentals=0)


def lane_take(values, index):
    return jnp.take_along_axis(values, index, axis=1, mode="promise_in_bounds")


def split3(values):
    high = values.astype(jnp.bfloat16)
    rest = values - high.astype(jnp.float32)
    middle = rest.astype(jnp.bfloat16)
    low = (rest - middle.astype(jnp.float32)).astype(jnp.bfloat16)
    return high, middle, low


def nn_dot(a, b):
    return lax.dot_general(a, b, (((1,), (0,)), ((), ())), preferred_element_type=jnp.float32)


def block_rows(blocks, tiles, rows):
    safe = jnp.maximum(blocks, 0)
    return jnp.where(blocks >= 0, (safe % tiles) * rows + safe // tiles, -1)


def inverse_rows(cols):
    lane = lax.broadcasted_iota(jnp.int32, (8, LANES), 1)
    sub = lax.broadcasted_iota(jnp.int32, (8, LANES), 0)
    order = (lane + 1).astype(jnp.float32)
    index = (lane % 16) * 8 + sub
    group = lane // 16
    high = jnp.right_shift(cols, 4)
    low = jnp.bitwise_and(cols, 15)
    left = jnp.concatenate([jnp.where(high == h, 1.0, 0.0) for h in range(8)], axis=0)
    right = jnp.concatenate([jnp.where(low == b, order, 0.0) for b in range(16)], axis=0)
    product = lax.dot_general(
        left.astype(jnp.bfloat16),
        right.astype(jnp.bfloat16),
        (((1,), (1,)), ((), ())),
        preferred_element_type=jnp.float32,
    )
    found = jnp.zeros((8, LANES), jnp.float32)
    for h in range(8):
        found = jnp.where(group == h, lane_take(product[h * 8 : (h + 1) * 8], index), found)
    return found.astype(jnp.int32) - 1


def ice_block(mass, coriolis, start, wind, current):
    pairs, width = mass.shape
    lane = lax.broadcasted_iota(jnp.int32, (pairs, width), 1)
    first, last = lane == 0, lane == width - 1

    def beside(values):
        before = jnp.where(first, 0.0, pltpu.roll(values, 1, 1))
        after = jnp.where(last, 0.0, pltpu.roll(values, width - 1, 1))
        return before + after

    diagonal = mass + drag_coeff + 2.0 * link_coeff
    turning = coriolis * mass
    inverse = 1.0 / (diagonal * diagonal + turning * turning)
    diagonal = diagonal * inverse
    turning = turning * inverse
    east, north = start
    base_east = mass * east + wind[0] + drag_coeff * current[0]
    base_north = mass * north + wind[1] + drag_coeff * current[1]
    for _ in range(ICE_SWEEPS):
        right_east = base_east + link_coeff * beside(east)
        right_north = base_north + link_coeff * beside(north)
        east = diagonal * right_east + turning * right_north
        north = diagonal * right_north - turning * right_east
    return east, north


def neighbour_copies(sizes, moves, send, recv):
    nz, nm = sizes
    z, m = lax.axis_index("zon"), lax.axis_index("mer")
    return [
        pltpu.make_async_remote_copy(
            src_ref=source,
            dst_ref=target,
            send_sem=send.at[i],
            recv_sem=recv.at[i],
            device_id={"zon": lax.rem(z + dz + nz, nz), "mer": lax.rem(m + dm + nm, nm)},
            device_id_type=pl.DeviceIdType.MESH,
        )
        for i, (source, target, dz, dm) in enumerate(moves)
    ]


def pick_group(base, per, turned_ids, parts, cols_ref, values_ref, lanes_ref, group):
    pairs = cols_ref.shape[1]
    lane = lax.broadcasted_iota(jnp.int32, (LANES, LANES), 1)
    turned = jnp.concatenate(
        [
            lane_take(turned_ids, jnp.full((pairs, LANES), base + d, jnp.int32))
            for d in range(per)
        ],
        axis=0,
    )
    lanes_ref[group] = jnp.transpose(turned)[:8]
    pick = jnp.concatenate(
        [
            jnp.where(turned == lane + b * LANES, 1.0, 0.0).astype(jnp.bfloat16)
            for b in range(parts.shape[1] // LANES)
        ],
        axis=1,
    )
    picked = nn_dot(pick, parts[0]) + nn_dot(pick, parts[1]) + nn_dot(pick, parts[2])
    cols = cols_ref[pl.ds(base, per)].reshape(LANES, LANES)
    index = jnp.maximum(cols, 0)
    for c in range(2):
        taken = lane_take(picked[:, c * LANES : (c + 1) * LANES], index)
        taken = jnp.where(cols >= 0, taken, 0.0)
        for d in range(per):
            values_ref[base + d, c] = taken[d * pairs : (d + 1) * pairs]


def put_group(base, per, returned_ref, inverse_ref, put_ref, group):
    pairs = inverse_ref.shape[1]
    put = put_ref[group]
    inverse = inverse_ref[pl.ds(base, per)].reshape(LANES, LANES)
    index = jnp.maximum(inverse, 0)
    halves = []
    for c in range(2):
        values = jnp.concatenate([returned_ref[base + d, c] for d in range(per)], axis=0)
        halves.append(jnp.where(inverse >= 0, lane_take(values, index), 0.0))
    return nn_dot(
        jnp.concatenate([put] * 3, axis=1),
        jnp.concatenate(split3(jnp.concatenate(halves, axis=1)), axis=0),
    )


def pack_late(total, edge_ref, rows):
    parts = LANES // (2 * COL_RIM)
    deep = rows // parts
    per = LANES // COL_RIM
    slot = lax.broadcasted_iota(jnp.int32, (deep, LANES), 1) // COL_RIM
    first = jnp.zeros((deep, LANES), jnp.float32)
    last = first
    for spot in range(per):
        at = (spot // 2) * deep
        lanes = slice(spot % 2 * LANES, (spot % 2 + 1) * LANES)
        head = total[at : at + deep, lanes]
        tail = total[total.shape[0] - rows + at : total.shape[0] - rows + at + deep, lanes]
        if spot:
            head = pltpu.roll(head, spot * COL_RIM, 1)
        if spot != per - 1:
            tail = pltpu.roll(tail, (spot + 1) * COL_RIM, 1)
        first = jnp.where(slot == spot, head, first)
        last = jnp.where(slot == spot, tail, last)
    edge_ref[0] = first
    edge_ref[1] = last


def late_moves(sizes, stress_ref, edge_ref, east_ref, west_ref, south_ref, north_ref, send, recv):
    rows, deep = stress_ref.shape[1], edge_ref.shape[1]

    def part(at, count=ROW_RIM):
        return pl.ds(at, count)

    return neighbour_copies(
        sizes,
        [
            (edge_ref.at[0], east_ref.at[part(0, deep)], -1, 0),
            (edge_ref.at[1], west_ref.at[part(0, deep)], 1, 0),
            (edge_ref.at[0, part(0)], east_ref.at[part(deep)], -1, -1),
            (edge_ref.at[0, part(deep - ROW_RIM)], east_ref.at[part(deep + ROW_RIM)], -1, 1),
            (edge_ref.at[1, part(0)], west_ref.at[part(deep)], 1, -1),
            (edge_ref.at[1, part(deep - ROW_RIM)], west_ref.at[part(deep + ROW_RIM)], 1, 1),
            (stress_ref.at[:, part(0)], south_ref, 0, -1),
            (stress_ref.at[:, part(rows - ROW_RIM)], north_ref, 0, 1),
        ],
        send,
        recv,
    )


def late_tile(c, east_ref, west_ref, known):
    per = LANES // COL_RIM
    parts = per // 2
    deep = east_ref.shape[0] - 2 * ROW_RIM

    def spread(ref, target):
        spots = [(0, deep, 2 * q + c) for q in range(parts)]
        spots += [(deep, ROW_RIM, c), (deep + ROW_RIM, ROW_RIM, 2 * parts - 2 + c)]
        pieces = []
        for at, count, spot in spots:
            shift = (target - spot) % per * COL_RIM
            piece = ref[at : at + count]
            pieces.append(pltpu.roll(piece, shift, 1) if shift else piece)
        return jnp.concatenate(pieces, axis=0)

    east = spread(east_ref, 0)
    west = spread(west_ref, per - 1)
    slot = lax.broadcasted_iota(jnp.int32, east.shape, 1) // COL_RIM
    both = jnp.where(slot == 0, east, jnp.where(slot == per - 1, west, 0.0))
    return jnp.where(known, both, 0.0)


def known_rows(sizes, rows, tall):
    m = lax.axis_index("mer")
    row = lax.broadcasted_iota(jnp.int32, (tall, LANES), 0)
    lower = jnp.where(m == sizes[1] - 1, rows, rows + ROW_RIM)
    upper = jnp.where(m == 0, tall, rows + ROW_RIM)
    return (row < lower) | ((row >= rows + ROW_RIM) & (row >= upper))


def split_columns(tiles):
    rows = tiles[0].shape[0]
    lane = lax.broadcasted_iota(jnp.int32, (rows, LANES), 1)
    half = LANES // 2
    index = 2 * (lane % half) + lane // half
    low = lane < half
    here = [lane_take(tile, index) for tile in tiles]
    away = [pltpu.roll(tile, half, 1) for tile in here]
    even, odd = [], []
    for t in range(0, len(tiles), 2):
        u = min(t + 1, len(tiles) - 1)
        even.append(jnp.where(low, here[t], away[u]))
        odd.append(jnp.where(low, away[t], here[u]))
    return even, odd


def join_columns(even, odd, tile):
    rows = even.shape[0]
    lane = lax.broadcasted_iota(jnp.int32, (rows, LANES), 1)
    index = (tile % 2) * (LANES // 2) + lane // 2
    return jnp.where(lane % 2 == 0, lane_take(even, index), lane_take(odd, index))


def rim_lanes(arrays):
    order = [k for k in range(arrays) if k != FIELD] + [FIELD]
    return [(k, i * EAST_COLS, i * WEST_COLS) for i, k in enumerate(order)]


def pack_rims(body_ref, edge_ref):
    arrays, rows, width = body_ref.shape
    lane = lax.broadcasted_iota(jnp.int32, (rows, LANES), 1)
    first = jnp.zeros((rows, LANES), jnp.float32)
    last = first
    for k, east, west in rim_lanes(arrays):
        head = body_ref[k, :, :LANES]
        tail = body_ref[k, :, width - LANES :]
        if east:
            head = pltpu.roll(head, east, 1)
        first = jnp.where(lane >= east, head, first)
        if k == FIELD:
            last = jnp.where(lane >= west, tail, last)
        else:
            tail = pltpu.roll(tail, west + WEST_COLS, 1)
            last = jnp.where((lane >= west) & (lane < west + WEST_COLS), tail, last)
    edge_ref[0, :rows] = first
    edge_ref[1, :rows] = last
    near = lane[:ROW_RIM]
    extra = jnp.zeros((ROW_RIM, LANES), jnp.float32)
    for g in range(rows // ROW_RIM):
        piece = body_ref[FIELD, g * ROW_RIM : (g + 1) * ROW_RIM, width - LANES :]
        at = g * EXTRA_COLS
        shift = (at + COL_RIM) % LANES
        if shift:
            piece = pltpu.roll(piece, shift, 1)
        extra = jnp.where((near >= at) & (near < at + EXTRA_COLS), piece, extra)
    edge_ref[1, rows : rows + ROW_RIM] = extra
    edge_ref[0, rows : rows + ROW_RIM] = extra


def rim_moves(sizes, body_ref, edge_ref, east_ref, west_ref, south_ref, north_ref, send, recv):
    rows = body_ref.shape[1]
    end = rows - ROW_RIM

    def part(at, count=ROW_RIM):
        return pl.ds(at, count)

    return neighbour_copies(
        sizes,
        [
            (edge_ref.at[0, part(0, rows)], east_ref.at[part(0, rows)], -1, 0),
            (edge_ref.at[1], west_ref.at[part(0, rows + ROW_RIM)], 1, 0),
            (body_ref.at[:, part(0)], south_ref, 0, -1),
            (body_ref.at[:, part(end)], north_ref, 0, 1),
            (edge_ref.at[0, part(0)], east_ref.at[part(rows)], -1, -1),
            (edge_ref.at[0, part(end)], east_ref.at[part(rows + ROW_RIM)], -1, 1),
            (edge_ref.at[1, part(0)], west_ref.at[part(rows + ROW_RIM)], 1, -1),
            (edge_ref.at[1, part(end)], west_ref.at[part(rows + 2 * ROW_RIM)], 1, 1),
            (edge_ref.at[1, part(rows)], west_ref.at[part(rows + 3 * ROW_RIM)], 1, -1),
            (edge_ref.at[1, part(rows)], west_ref.at[part(rows + 4 * ROW_RIM)], 1, 1),
        ],
        send,
        recv,
    )


def extra_columns(west_ref, rows):
    pieces = []
    for g in range(rows // ROW_RIM):
        shift = (2 * LANES - COL_RIM - g * EXTRA_COLS) % LANES
        piece = west_ref[rows : rows + ROW_RIM]
        pieces.append(pltpu.roll(piece, shift, 1) if shift else piece)
    south = west_ref[rows + 3 * ROW_RIM : rows + 4 * ROW_RIM]
    north = west_ref[rows + 4 * ROW_RIM : rows + 5 * ROW_RIM]
    pieces.append(pltpu.roll(south, LANES - COL_RIM, 1))
    last = (2 * LANES - COL_RIM - (rows // ROW_RIM - 1) * EXTRA_COLS) % LANES
    pieces.append(pltpu.roll(north, last, 1) if last else north)
    return jnp.concatenate(pieces, axis=0)


def rim_tile(k, east_at, west_at, east_ref, west_ref, extra, rows, known):
    tall = rows + 2 * ROW_RIM
    lane = lax.broadcasted_iota(jnp.int32, (tall, LANES), 1)
    east = east_ref[...]
    west = jnp.concatenate(
        [west_ref[:rows], west_ref[rows + ROW_RIM : rows + 3 * ROW_RIM]], axis=0
    )
    if east_at:
        east = pltpu.roll(east, LANES - east_at, 1)
    if k == FIELD:
        kept, near = EAST_COLS + 1, LANES - (LANES - west_at)
        west = jnp.where(lane >= near, west, extra)
        first = LANES - COL_RIM
    else:
        kept, first = EAST_COLS, LANES - WEST_COLS
        west = pltpu.roll(west, LANES - west_at - WEST_COLS, 1)
    both = jnp.where(lane < kept, east, jnp.where(lane >= first, west, 0.0))
    return jnp.where(known, both, 0.0)


def travel_kernel(
    sizes,
    current_hbm, blocks_hbm, cols_hbm, mass_hbm, coriolis_hbm, start_hbm, wind_hbm,
    sea_hbm, forcing_hbm, weights_hbm, excess_hbm, mask_hbm,
    velocity_ref, halves_ref, stress_ref, late_east, late_west, late_south, late_north,
    current_ref, blocks_ref, square, cols_ref, mass_ref, coriolis_ref, start_ref, wind_ref,
    sea_ref, forcing_ref, weights_ref, excess_ref, mask_ref,
    parts, lanes_ref, put_ref, values_ref, arrived, drag, returned_ref, inverse_ref, total,
    body_ref, edge, east_ref, west_ref, south_ref, north_ref, field, stress_edge,
    loads, send_out, recv_out, send_back, recv_back, send_rim, recv_rim, send_late, recv_late,
):
    nz, nm = sizes
    count = nz * nm
    z, m = lax.axis_index("zon"), lax.axis_index("mer")
    me = z * nm + m
    _, rows, width = current_ref.shape
    tiles = width // LANES
    devices, pairs, _ = cols_ref.shape
    per = LANES // pairs
    span = per // nm
    groups = count // per
    mine = lax.div(z, span)

    def group_of(i):
        return lax.rem(mine + groups // 2 + lax.div(i + 1, 2) * (1 - 2 * lax.rem(i, 2)), groups)

    def group_from(i):
        return lax.rem(
            mine + groups + groups // 2 - lax.div(i + 1, 2) * (1 - 2 * lax.rem(i, 2)), groups
        )

    def member(group, k):
        inner = lax.rem(k, per)
        a = lax.rem(lax.rem(z, span) + span - 1 - lax.div(inner, nm), span)
        return group * span + a, lax.rem(m + nm - 1 - lax.rem(inner, nm), nm)

    def member_from(group, k):
        inner = lax.rem(k, per)
        a = lax.rem(lax.rem(z, span) + 1 + lax.div(inner, nm), span)
        return group * span + a, lax.rem(m + 1 + lax.rem(inner, nm), nm)

    def ahead(k):
        return member(group_of(lax.div(k, per)), k)

    def behind(k):
        return member_from(group_from(lax.div(k, per)), k)

    def out_copy(k):
        pz, pm = ahead(k)
        return pltpu.make_async_remote_copy(
            src_ref=values_ref.at[pz * nm + pm],
            dst_ref=arrived.at[me],
            send_sem=send_out.at[k],
            recv_sem=recv_out.at[k],
            device_id={"zon": pz, "mer": pm},
            device_id_type=pl.DeviceIdType.MESH,
        )

    def back_copy(k):
        pz, pm = behind(k)
        return pltpu.make_async_remote_copy(
            src_ref=drag.at[k],
            dst_ref=returned_ref.at[me],
            send_sem=send_back.at[k],
            recv_sem=recv_back.at[k],
            device_id={"zon": pz, "mer": pm},
            device_id_type=pl.DeviceIdType.MESH,
        )

    barrier = pltpu.get_barrier_semaphore()

    def greet(k, carry):
        pz, pm = ahead(k)
        pl.semaphore_signal(
            barrier,
            inc=1,
            device_id={"zon": pz, "mer": pm},
            device_id_type=pl.DeviceIdType.MESH,
        )
        return carry

    copies = [
        pltpu.make_async_copy(source, target, loads.at[i])
        for i, (source, target) in enumerate(
            [
                (current_hbm, current_ref),
                (blocks_hbm.at[0], blocks_ref),
                (cols_hbm.at[0], cols_ref),
                (mass_hbm.at[0], mass_ref),
                (coriolis_hbm.at[0], coriolis_ref),
                (start_hbm.at[:, 0], start_ref),
                (wind_hbm.at[:, 0], wind_ref),
                (weights_hbm, weights_ref),
                (sea_hbm, sea_ref),
                (forcing_hbm, forcing_ref),
                (excess_hbm, excess_ref),
                (mask_hbm, mask_ref),
            ]
        )
    ]
    for copy in copies:
        copy.start()
    lax.fori_loop(0, count - 1, greet, 0)

    copies[0].wait()
    for j in range(tiles):
        for c in range(2):
            for k, part in enumerate(split3(current_ref[c, :, j * LANES : (j + 1) * LANES])):
                parts[k, j * rows : (j + 1) * rows, c * LANES : (c + 1) * LANES] = part
    copies[1].wait()
    square[:devices, :pairs] = block_rows(blocks_ref[...], tiles, rows)
    turned_ids = jnp.transpose(square[...])[:pairs]
    copies[2].wait()

    def pick(i, carry):
        group = group_of(i)
        pick_group(group * per, per, turned_ids, parts, cols_ref, values_ref, lanes_ref, group)
        return carry

    def launch(k, carry):
        out_copy(k).start()
        return carry

    first = min(2, groups)
    lax.fori_loop(0, first, pick, 0)
    pl.semaphore_wait(barrier, count - 1)

    def pick_and_launch(i, carry):
        lax.fori_loop((i - first) * per, (i - first + 1) * per, launch, 0)
        return pick(i, carry)

    lax.fori_loop(first, groups, pick_and_launch, 0)
    lax.fori_loop((groups - first) * per, count - 1, launch, 0)

    for copy in copies[3:]:
        copy.wait()
    prepare_kernel(sea_ref, forcing_ref, weights_ref, excess_ref, mask_ref, body_ref, edge)

    def ice(at, from_ref):
        current = (from_ref[at, 0], from_ref[at, 1])
        east, north = ice_block(
            mass_ref[at],
            coriolis_ref[at],
            (start_ref[0, at], start_ref[1, at]),
            (wind_ref[0, at], wind_ref[1, at]),
            current,
        )
        velocity_ref[0, at] = east
        velocity_ref[1, at] = north
        return drag_coeff * (east - current[0]), drag_coeff * (north - current[1])

    def invert(k):
        for r in range(0, pairs, 8):
            inverse_ref[k, r : r + 8] = inverse_rows(cols_ref[k, r : r + 8])

    own_east, own_north = ice(me, values_ref)
    invert(count - 1)
    returned_ref[me, 0] = own_east
    returned_ref[me, 1] = own_north

    rim = rim_moves(
        sizes, body_ref, edge, east_ref, west_ref, south_ref, north_ref, send_rim, recv_rim
    )
    for copy in rim:
        copy.start()

    def step(k, carry):
        out_copy(k).wait_recv()
        pz, pm = behind(k)
        east, north = ice(pz * nm + pm, arrived)
        drag[k, 0] = east
        drag[k, 1] = north
        invert(k)

        @pl.when(k > 0)
        def _():
            back_copy(k - 1).start()

        return carry

    lax.fori_loop(0, count - 1, step, 0)
    back_copy(count - 2).start()

    for copy in rim:
        copy.wait()
    tall, wide = rows + 2 * ROW_RIM, width + LANES
    half = tall // 2
    wide_tiles = wide // LANES
    known = known_rows(sizes, rows, tall)
    has_south, has_north = m < nm - 1, m > 0
    extra = extra_columns(west_ref, rows)
    for k, east_at, west_at in rim_lanes(body_ref.shape[0]):
        for t in range(tiles):
            part = slice(t * LANES, (t + 1) * LANES)
            field[t, :rows] = body_ref[k, :, part]
            field[t, rows : rows + ROW_RIM] = jnp.where(has_south, south_ref[k, :, part], 0.0)
            field[t, rows + ROW_RIM :] = jnp.where(has_north, north_ref[k, :, part], 0.0)
        field[tiles] = rim_tile(k, east_at, west_at, east_ref, west_ref, extra, rows, known)
        for which in range(2):
            rows_of = pl.ds(which, half, stride=2)
            split = split_columns([field[t, rows_of, :] for t in range(wide_tiles)])
            for odd, found in enumerate(split):
                whole = jnp.concatenate(found, axis=1)
                if k in (4, 6) and odd:
                    whole = pltpu.roll(whole, 1, 1)
                if k in (5, 7) and not odd:
                    whole = pltpu.roll(whole, whole.shape[1] - 1, 1)
                halves_ref[k, which, odd] = whole

    total[...] = jnp.zeros_like(total)
    row = lax.broadcasted_iota(jnp.int32, (rows * tiles, LANES), 0)

    def place(group, carry):
        ids = jnp.broadcast_to(lanes_ref[group][:1], row.shape)
        put_ref[group] = jnp.where(ids == row, 1.0, 0.0).astype(jnp.bfloat16)
        return carry

    lax.fori_loop(0, groups, place, 0)

    def collect(turn, carry):
        i = lax.rem(turn + groups - 1, groups)
        group = group_of(i)

        def arrive(k, inner):
            back_copy(k).wait_recv()
            return inner

        lax.fori_loop(i * per, jnp.minimum(i * per + per, count - 1), arrive, 0)
        added = put_group(
            group * per, per, returned_ref, inverse_ref, put_ref, group
        )

        total[...] += added
        return carry

    lax.fori_loop(0, groups, collect, 0)
    pack_late(total, stress_edge, rows)
    for c in range(2):
        for j in range(tiles):
            stress_ref[c, :, j * LANES : (j + 1) * LANES] = total[
                j * rows : (j + 1) * rows, c * LANES : (c + 1) * LANES
            ]
    late = late_moves(
        sizes, stress_ref, stress_edge, late_east, late_west, late_south, late_north,
        send_late, recv_late,
    )
    for copy in late:
        copy.start()

    def finish(k, carry):
        out_copy(k).wait_send()
        back_copy(k).wait_send()
        return carry

    lax.fori_loop(0, count - 1, finish, 0)
    for copy in late:
        copy.wait()


def prepare_kernel(sea_ref, forcing_ref, weights_ref, excess_ref, mask_ref, out_ref, edge_ref):
    total = weights_ref[0]
    for k in range(1, 8):
        total = total + weights_ref[k]
    ocean = mask_ref[...] > 0
    inverse = jnp.where(ocean, 1.0 / ((1.0 + excess_ref[...]) * total), 0.0)
    for k in range(8):
        out_ref[k] = weights_ref[k] * inverse
    out_ref[8] = inverse
    out_ref[9] = jnp.where(ocean, sea_ref[...], 0.0)
    out_ref[10] = forcing_ref[...]
    pack_rims(out_ref, edge_ref)


def sweep_kernel(
    sizes,
    halves_ref, stress_ref, late_east, late_west, late_south, late_north, velocity_ref,
    out_ref, velocity_hbm,
    wide_ref, tile_ref, source_ref, field_ref, write,
):
    _, rows, width = stress_ref.shape
    tall, wide = rows + 2 * ROW_RIM, width + LANES
    half = tall // 2
    tiles = wide // LANES
    write_velocity = pltpu.make_async_copy(velocity_ref, velocity_hbm, write)
    write_velocity.start()
    m = lax.axis_index("mer")
    has_south, has_north = m < sizes[1] - 1, m > 0
    known = known_rows(sizes, rows, tall)
    for c in range(2):
        wide_ref[c, :rows, :width] = stress_ref[c]
        wide_ref[c, rows : rows + ROW_RIM, :width] = jnp.where(has_south, late_south[c], 0.0)
        wide_ref[c, rows + ROW_RIM :, :width] = jnp.where(has_north, late_north[c], 0.0)
        wide_ref[c, :, width:] = late_tile(c, late_east, late_west, known)
    east_stress = wide_ref[0]
    north_stress = wide_ref[1]
    change = (
        pltpu.roll(north_stress, wide - 1, 1)
        - pltpu.roll(north_stress, 1, 1)
        - pltpu.roll(east_stress, tall - 1, 0)
        + pltpu.roll(east_stress, 1, 0)
    )
    for t in range(tiles):
        tile_ref[t] = change[:, t * LANES : (t + 1) * LANES]

    thin = field_ref.shape[3]
    for which in range(2):
        rows_of = pl.ds(which, half, stride=2)
        split = split_columns([tile_ref[t, rows_of, :] for t in range(tiles)])
        for odd, found in enumerate(split):
            source_ref[which, odd] = (
                halves_ref[10, which, odd] + jnp.concatenate(found, axis=1)
            ) * halves_ref[8, which, odd]
            field_ref[which, odd] = halves_ref[FIELD, which, odd]

    def phase(which, colours):
        other = [field_ref[1 - which, odd] for odd in range(2)]
        if which:
            above = other
            below = [pltpu.roll(value, half - 1, 0) for value in other]
        else:
            above = [pltpu.roll(value, 1, 0) for value in other]
            below = other
        weight = [[halves_ref[k, which, odd] for k in range(8)] for odd in range(2)]
        w = weight[0]
        base_even = source_ref[which, 0] + w[2] * below[0] + w[3] * above[0]
        base_even = base_even + w[4] * below[1] + w[6] * above[1]
        base_even = base_even + pltpu.roll(w[5] * below[1] + w[7] * above[1], 1, 1)
        w = weight[1]
        base_odd = source_ref[which, 1] + w[2] * below[1] + w[3] * above[1]
        base_odd = base_odd + w[5] * below[0] + w[7] * above[0]
        base_odd = base_odd + pltpu.roll(w[4] * below[0] + w[6] * above[0], thin - 1, 1)
        even, odd = field_ref[which, 0], field_ref[which, 1]
        for parity in colours:
            if parity:
                odd = base_odd + weight[1][0] * pltpu.roll(even, thin - 1, 1)
                odd = odd + weight[1][1] * even
            else:
                even = base_even + weight[0][0] * odd
                even = even + weight[0][1] * pltpu.roll(odd, 1, 1)
        field_ref[which, 0] = even
        field_ref[which, 1] = odd

    runs = [(0, [0, 1])]
    for _ in range(SWEEPS):
        runs += [(1, [0, 1, 0]), (0, [1, 0, 1])]
    runs[-1] = (0, [1, 0])
    for which, colours in runs:
        phase(which, colours)
    for t in range(tiles - 1):
        at = slice(t // 2 * LANES, t // 2 * LANES + LANES)
        for which in range(2):
            tile_ref[t, pl.ds(which, rows // 2, stride=2), :] = join_columns(
                field_ref[which, 0, : rows // 2, at], field_ref[which, 1, : rows // 2, at], t
            )
        out_ref[:, t * LANES : (t + 1) * LANES] = tile_ref[t, :rows, :]
    write_velocity.wait()


def local(
    sea_level,
    forcing,
    link_weights,
    excess,
    ocean_mask,
    current,
    intersection_block,
    intersection_cols,
    ice_mass,
    coriolis,
    ice_start,
    wind_stress,
):
    rows, width = sea_level.shape
    _, devices, pairs, block = intersection_cols.shape
    slots = devices * pairs
    tiles = width // LANES
    f32 = jnp.float32
    ice_shape = (devices, pairs, block)
    slot_bytes = slots * block * 4
    sizes = (lax.axis_size("zon"), lax.axis_size("mer"))
    arrays = 11
    tall, wide = rows + 2 * ROW_RIM, width + LANES
    thin = -(-wide // (2 * LANES)) * LANES
    deep = rows * 2 * COL_RIM // LANES
    dma = pltpu.SemaphoreType.DMA
    shape = jax.ShapeDtypeStruct
    stay = functools.partial(pltpu.with_memory_space_constraint, memory_space=pltpu.HBM)
    velocity, halves, *late = pl.pallas_call(
        functools.partial(travel_kernel, sizes),
        out_shape=(
            shape((2,) + ice_shape, f32),
            shape((arrays, 2, 2, tall // 2, thin), f32),
            shape((2, rows, width), f32),
            shape((deep + 2 * ROW_RIM, LANES), f32),
            shape((deep + 2 * ROW_RIM, LANES), f32),
            shape((2, ROW_RIM, width), f32),
            shape((2, ROW_RIM, width), f32),
        ),
        in_specs=[HBM] * 12,
        out_specs=(VM,) * 7,
        scratch_shapes=[
            pltpu.VMEM((2, rows, width), f32),
            pltpu.VMEM((devices, pairs), jnp.int32),
            pltpu.VMEM((LANES, LANES), jnp.int32),
            pltpu.VMEM(ice_shape, jnp.int32),
            pltpu.VMEM(ice_shape, f32),
            pltpu.VMEM(ice_shape, f32),
            pltpu.VMEM((2,) + ice_shape, f32),
            pltpu.VMEM((2,) + ice_shape, f32),
            pltpu.VMEM((rows, width), f32),
            pltpu.VMEM((rows, width), f32),
            pltpu.VMEM((8, rows, width), f32),
            pltpu.VMEM((rows, width), f32),
            pltpu.VMEM((rows, width), jnp.int32),
            pltpu.VMEM((3, rows * tiles, 2 * LANES), jnp.bfloat16),
            pltpu.VMEM((slots // LANES, 8, LANES), jnp.int32),
            pltpu.VMEM((slots // LANES, rows * tiles, LANES), jnp.bfloat16),
            pltpu.VMEM((devices, 2, pairs, block), f32),
            pltpu.VMEM((devices, 2, pairs, block), f32),
            pltpu.VMEM((devices, 2, pairs, block), f32),
            pltpu.VMEM((devices, 2, pairs, block), f32),
            pltpu.VMEM(ice_shape, jnp.int32),
            pltpu.VMEM((rows * tiles, 2 * LANES), f32),
            pltpu.VMEM((arrays, rows, width), f32),
            pltpu.VMEM((2, rows + ROW_RIM, LANES), f32),
            pltpu.VMEM((tall, LANES), f32),
            pltpu.VMEM((rows + 5 * ROW_RIM, LANES), f32),
            pltpu.VMEM((arrays, ROW_RIM, width), f32),
            pltpu.VMEM((arrays, ROW_RIM, width), f32),
            pltpu.VMEM((wide // LANES, tall, LANES), f32),
            pltpu.VMEM((2, deep, LANES), f32),
            dma((12,)),
            dma((devices,)),
            dma((devices,)),
            dma((devices,)),
            dma((devices,)),
            dma((10,)),
            dma((10,)),
            dma((8,)),
            dma((8,)),
        ],
        compiler_params=pltpu.CompilerParams(
            vmem_limit_bytes=TRAVEL_VMEM, collective_id=0, has_side_effects=True
        ),
        cost_estimate=cost(slots * block * 4096, 16 * slot_bytes),
        name="travel",
    )(
        stay(current),
        stay(intersection_block),
        stay(intersection_cols),
        stay(ice_mass),
        stay(coriolis),
        stay(ice_start),
        stay(wind_stress),
        stay(sea_level),
        stay(forcing),
        stay(link_weights),
        stay(excess),
        stay(ocean_mask),
    )
    surface, velocity = pl.pallas_call(
        functools.partial(sweep_kernel, sizes),
        out_shape=(shape((rows, width), f32), shape((2,) + ice_shape, f32)),
        in_specs=[VM] * 7,
        out_specs=(VM, HBM),
        scratch_shapes=[
            pltpu.VMEM((2, tall, wide), f32),
            pltpu.VMEM((wide // LANES, tall, LANES), f32),
            pltpu.VMEM((2, 2, tall // 2, thin), f32),
            pltpu.VMEM((2, 2, tall // 2, thin), f32),
            dma,
        ],
        compiler_params=pltpu.CompilerParams(vmem_limit_bytes=SWEEP_VMEM),
        cost_estimate=cost(rows * width * 200, rows * width * 64),
        name="sweep",
    )(halves, *late, velocity)
    return (surface, velocity.reshape((2, 1) + ice_shape))


def solution(mesh):
    return jax.shard_map(
        local,
        mesh=mesh,
        in_specs=(
            P("mer", "zon"),
            P("mer", "zon"),
            P(None, "mer", "zon"),
            P("mer", "zon"),
            P("mer", "zon"),
            P(None, "mer", "zon"),
            P(("zon", "mer"), None, None),
            P(("zon", "mer"), None, None, None),
            P(("zon", "mer"), None, None, None),
            P(("zon", "mer"), None, None, None),
            P(None, ("zon", "mer"), None, None, None),
            P(None, ("zon", "mer"), None, None, None),
        ),
        out_specs=(P("mer", "zon"), P(None, ("zon", "mer"), None, None, None)),
        check_vma=False,
    )
```
